32 devices in a mesh: data: 32 (over z, y, x, core).
Axes of the slice: x: 2, y: 2, z: 4, core: 2. Of those that a mesh axis runs over, the one named last changes fastest.
Arguments:
- x_in: bfloat16 [131072, 768], P('data')
- d_out: bfloat16 [131072, 768], P('data')
- w_stack: bfloat16 [4, 768, 768], replicated
- a_old: float32 [4, 768, 768], replicated
- s_old: float32 [4, 768, 768], replicated
- a_inv: float32 [4, 768, 768], replicated
- s_inv: float32 [4, 768, 768], replicated
Outputs:
- output 1: float32 [4, 768, 768], replicated
- output 2: float32 [4, 768, 768], replicated
- output 3: float32 [4, 768, 768], replicated
All inputs are finite; a program needn't handle non-finite values.
Results may differ from the reference program's by a relative error of at most 0.00117834.
Values are sent between devices in bfloat16 or wider.
A program may use at most 1 GiB of HBM per device.

```python
import jax
import jax.numpy as jnp
from jax import lax

D = 768
LAYERS = 4
TOK_DEV = 4096
GROUP = 32
RANK = 64
TOKENS = TOK_DEV * GROUP
RHO = 0.75
ERF_SCALE = 0.7071067811865476
PDF_SCALE = 0.3989422804014327


def gelu_fwd(z_val):
    return 0.5 * z_val * (1.0 + lax.erf(z_val * ERF_SCALE))


def gelu_slope(z_val):
    return 0.5 * (1.0 + lax.erf(z_val * ERF_SCALE)) + z_val * jnp.exp(-0.5 * z_val * z_val) * PDF_SCALE


def tok_gram(lhs_rows, rhs_rows):
    return lax.dot_general(lhs_rows, rhs_rows, (((0,), (0,)), ((), ())), preferred_element_type=jnp.float32)


def sharded_rows(key_list, base_size, own_size, mix_lo, mix_hi, scale_lo, scale_hi):
    noise_rows = jax.random.normal(key_list[0], (GROUP, TOK_DEV, D), jnp.float32)
    base_dir = jax.random.normal(key_list[1], (1, D), jnp.float32) * base_size
    mixing = jax.random.uniform(key_list[2], (GROUP, 1), jnp.float32, mix_lo, mix_hi)
    own_shift = jax.random.normal(key_list[3], (GROUP, D), jnp.float32) * own_size
    shard_scale = jax.random.uniform(key_list[4], (GROUP, 1, 1), jnp.float32, scale_lo, scale_hi)
    row_shift = mixing * base_dir + own_shift
    drawn_rows = noise_rows * shard_scale + row_shift[:, None, :]
    return drawn_rows.reshape(TOKENS, D).astype(jnp.bfloat16)


def old_factor(key_one, diag_lo, diag_hi, spread):
    key_pair = jax.random.split(key_one, 2)
    diag_vals = jax.random.uniform(key_pair[0], (LAYERS, D), jnp.float32, diag_lo, diag_hi)
    basis_mat = jax.random.normal(key_pair[1], (LAYERS, D, RANK), jnp.float32) * spread
    low_rank = jnp.einsum("lik,ljk->lij", basis_mat, basis_mat)
    return low_rank + diag_vals[:, :, None] * jnp.eye(D, dtype=jnp.float32)


def inv_factor(key_one, spread):
    key_pair = jax.random.split(key_one, 2)
    raw_draw = jax.random.normal(key_pair[0], (LAYERS, D, D), jnp.float32)
    diag_vals = jax.random.uniform(key_pair[1], (LAYERS, D), jnp.float32, 0.7, 1.5)
    sym_part = (raw_draw + jnp.swapaxes(raw_draw, 1, 2)) * (spread * D ** -0.5)
    return sym_part + diag_vals[:, :, None] * jnp.eye(D, dtype=jnp.float32)


def setup_inputs(seed: int = 0) -> dict:
    key_list = jax.random.split(jax.random.key(seed), 15)
    x_in = sharded_rows(key_list[0:5], 0.8, 0.5, 0.2, 1.0, 0.6, 1.4)
    d_out = sharded_rows(key_list[5:10], 0.6, 0.4, -0.5, 1.0, 0.5, 1.5)
    w_draw = jax.random.normal(key_list[10], (LAYERS, D, D), jnp.float32) * D ** -0.5
    return {"x_in": x_in, "d_out": d_out, "w_stack": w_draw.astype(jnp.bfloat16), "a_old": old_factor(key_list[11], 0.3, 1.2, 0.08), "s_old": old_factor(key_list[12], 0.2, 0.8, 0.06), "a_inv": inv_factor(key_list[13], 0.15), "s_inv": inv_factor(key_list[14], 0.15)}


def reference(x_in, d_out, w_stack, a_old, s_old, a_inv, s_inv):
    layer_in = []
    pre_act = []
    h_cur = x_in
    for layer_idx in range(LAYERS):
        layer_in.append(h_cur)
        z_cur = jnp.dot(h_cur, w_stack[layer_idx], preferred_element_type=jnp.float32).astype(jnp.bfloat16)
        pre_act.append(z_cur)
        if layer_idx < LAYERS - 1:
            h_cur = gelu_fwd(z_cur.astype(jnp.float32)).astype(jnp.bfloat16)
    a_list = []
    s_list = []
    w_list = []
    g_cur = d_out
    for layer_idx in reversed(range(LAYERS)):
        if layer_idx < LAYERS - 1:
            g_cur = (dh_cur.astype(jnp.float32) * gelu_slope(pre_act[layer_idx].astype(jnp.float32))).astype(jnp.bfloat16)
        h_prev = layer_in[layer_idx]
        a_list.append(tok_gram(h_prev, h_prev) / TOKENS)
        s_list.append(tok_gram(g_cur, g_cur) / TOKENS)
        w_list.append(tok_gram(h_prev, g_cur) / TOKENS)
        if layer_idx > 0:
            dh_cur = jnp.dot(g_cur, w_stack[layer_idx].T, preferred_element_type=jnp.float32).astype(jnp.bfloat16)
    a_stack = jnp.stack(a_list[::-1])
    s_stack = jnp.stack(s_list[::-1])
    w_grad = jnp.stack(w_list[::-1])
    left_mul = jnp.einsum("lij,ljk->lik", a_inv, w_grad, precision=lax.Precision.HIGHEST)
    u_stack = jnp.einsum("lij,ljk->lik", left_mul, s_inv, precision=lax.Precision.HIGHEST)
    return (u_stack, RHO * a_old + (1.0 - RHO) * a_stack, RHO * s_old + (1.0 - RHO) * s_stack)
```

```python
import functools

import jax
import jax.numpy as jnp
from jax import lax
from jax.experimental import pallas as pl
from jax.experimental.pallas import tpu as pltpu
from jax.sharding import PartitionSpec as P

RHO = 0.75
ERF_SCALE = 0.7071067811865476
PDF_SCALE = 0.3989422804014327

D = 768
BLK = 256
LAYERS = 4
UNIT = 256
MATS = 12
UNITS = 28
HALVINGS = 4
COPIES = 2 * HALVINGS + 1
RROWS = 256
MESH = pl.DeviceIdType.MESH
ORDERS = ((1, 2, 4, 8, 16), (1, 4, 2, 8, 16), (1, 8, 16, 2, 4))
CHUNKS = 4
DN0 = (((0,), (0,)), ((), ()))


def gelu_fwd(z_val):
    return 0.5 * z_val * (1.0 + lax.erf(z_val * ERF_SCALE))


def gelu_slope(z_val):
    return 0.5 * (1.0 + lax.erf(z_val * ERF_SCALE)) + z_val * jnp.exp(-0.5 * z_val * z_val) * PDF_SCALE


def times_wt(g_rows, w_mat):
    return lax.dot_general(g_rows, w_mat, (((1,), (1,)), ((), ())), preferred_element_type=jnp.float32)


def half_of(step):
    return 128 >> step


def land_of(step):
    return 256 - (256 >> step)


def reduce_kernel(inv_tokens, x, h1, h2, h3, g1, g2, g3, dy, ainv, sinv,
                  sym_out, u_out,
                  pay, rbuf, lbuf, gbuf, av, sv, ub,
                  ssem, rsem, fsem, lsem, gsem, isem, usem, osem):
    me = lax.axis_index("data")
    tok = x.shape[0]
    chunk = tok // CHUNKS
    acts = (x, h1, h2, h3)
    grads = (g1, g2, g3, dy)

    def bit(mask):
        return lax.rem(lax.div(me, mask), 2)

    def peer(mask):
        return me + mask * (1 - 2 * bit(mask))

    barrier = pltpu.get_barrier_semaphore()
    for mask in ORDERS[0]:
        pl.semaphore_signal(barrier, inc=1, device_id=(peer(mask),), device_id_type=MESH)
    pl.semaphore_wait(barrier, 5)

    def offset(order, step):
        off = 0
        for s in range(step):
            off = off + bit(order[s]) * half_of(s)
        return off

    def base_of(m):
        late = lax.div(m + 8, 12)
        return 3 * m - late * (m - 4)

    def rows_at(ref, start, size):
        return ref.at[pl.ds(pl.multiple_of(start, 8), size), :]

    def scatter_copy(m, j, step):
        order = ORDERS[j]
        unit = base_of(m) + j
        half = half_of(step)
        b = bit(order[step])
        src = unit * UNIT + offset(order, step) + (1 - b) * half
        return pltpu.make_async_remote_copy(
            src_ref=rows_at(pay, src, half),
            dst_ref=rows_at(rbuf, unit * RROWS + land_of(step), half),
            send_sem=ssem.at[m, j, step], recv_sem=rsem.at[m, j, step],
            device_id=(peer(order[step]),), device_id_type=MESH)

    def exchange_copy(m, j):
        order = ORDERS[j]
        unit = base_of(m) + j
        return pltpu.make_async_remote_copy(
            src_ref=rows_at(pay, unit * UNIT + offset(order, HALVINGS), 16),
            dst_ref=rows_at(rbuf, unit * RROWS + 240, 16),
            send_sem=ssem.at[m, j, HALVINGS], recv_sem=rsem.at[m, j, HALVINGS],
            device_id=(peer(order[HALVINGS]),), device_id_type=MESH)

    def gather_copy(m, j, step):
        order = ORDERS[j]
        unit = base_of(m) + j
        half = half_of(step)
        row = unit * UNIT + offset(order, step + 1)
        return pltpu.make_async_remote_copy(
            src_ref=rows_at(pay, row, half),
            dst_ref=rows_at(pay, row, half),
            send_sem=ssem.at[m, j, HALVINGS + 1 + step], recv_sem=rsem.at[m, j, HALVINGS + 1 + step],
            device_id=(peer(order[step]),), device_id_type=MESH)

    def give_back(m, j, step):
        pl.semaphore_signal(fsem.at[m, j, step], inc=1, device_id=(peer(ORDERS[j][step]),), device_id_type=MESH)

    def gather_start(m, j, step):
        pl.semaphore_wait(fsem.at[m, j, step], 1)
        gather_copy(m, j, step).start()

    def add_landed(m, j, step):
        order = ORDERS[j]
        unit = base_of(m) + j
        half = half_of(step) if step < HALVINGS else 16
        keep = unit * UNIT + offset(order, min(step + 1, HALVINGS))
        land = unit * RROWS + land_of(step)
        piece = min(half, 32)

        def one(i, carry):
            a = pl.ds(pl.multiple_of(keep + i * piece, 8), piece)
            c = pl.ds(pl.multiple_of(land + i * piece, 8), piece)
            pay[a, :] = pay[a, :] + rbuf[c, :]
            return carry

        if half == piece:
            one(0, 0)
        else:
            lax.fori_loop(0, half // piece, one, 0)

    def stage(k, m, j):
        if k <= HALVINGS:
            scatter_copy(m, j, k - 1).wait()
            give_back(m, j, k - 1)
            add_landed(m, j, k - 1)
            if k < HALVINGS:
                scatter_copy(m, j, k).start()
            else:
                exchange_copy(m, j).start()
        elif k == HALVINGS + 1:
            exchange_copy(m, j).wait()
            add_landed(m, j, HALVINGS)
            gather_start(m, j, HALVINGS - 1)
        else:
            step = COPIES - k
            gather_copy(m, j, step).wait()
            if step > 0:
                gather_start(m, j, step - 1)

    def wait_left(kc, slot):
        pltpu.make_async_copy(x.at[pl.ds(kc * chunk, chunk), :], lbuf.at[slot], lsem.at[slot]).wait()

    def wait_right(kc, slot):
        pltpu.make_async_copy(dy.at[pl.ds(kc * chunk, chunk), :], gbuf.at[slot], gsem.at[slot]).wait()

    def load(m, kc, slot):
        rows = pl.ds(kc * chunk, chunk)
        for i in range(MATS):
            if i < 4:
                left, right = acts[3 - i], grads[3 - i]
            else:
                left, right = (acts + grads)[i - 4], None

            @pl.when(m == i)
            def _(left=left, right=right):
                pltpu.make_async_copy(left.at[rows, :], lbuf.at[slot], lsem.at[slot]).start()
                if right is not None:
                    pltpu.make_async_copy(right.at[rows, :], gbuf.at[slot], gsem.at[slot]).start()

    def put(first, row, rows, c0, cols, val):
        a = pl.ds(pl.multiple_of(row, 8), rows)
        if first:
            pay[a, c0:c0 + cols] = val
        else:
            pay[a, c0:c0 + cols] = pay[a, c0:c0 + cols] + val

    def gram_dw(m):
        row = base_of(m) * UNIT
        for kc in range(CHUNKS):
            slot = kc % 2
            wait_left(kc, slot)
            wait_right(kc, slot)
            if kc + 1 < CHUNKS:
                load(m, kc + 1, 1 - slot)
            for j in range(3):
                val = lax.dot_general(lbuf[slot, :, j * BLK:(j + 1) * BLK], gbuf[slot], DN0,
                                      preferred_element_type=jnp.float32)
                put(kc == 0, row + j * UNIT, UNIT, 0, D, val)

    def gram_sym(m):
        row = base_of(m) * UNIT
        for kc in range(CHUNKS):
            slot = kc % 2
            wait_left(kc, slot)
            if kc + 1 < CHUNKS:
                load(m, kc + 1, 1 - slot)
            for j, (unit, c0) in enumerate(((0, 0), (1, 0), (1, 2 * BLK))):
                cols = D - j * BLK
                val = lax.dot_general(lbuf[slot, :, j * BLK:(j + 1) * BLK], lbuf[slot, :, j * BLK:], DN0,
                                      preferred_element_type=jnp.float32)
                put(kc == 0, row + unit * UNIT, UNIT, c0, cols, val)

    def inv_copies(m):
        layer = 3 - m
        return (pltpu.make_async_copy(ainv.at[layer], av, isem.at[0]),
                pltpu.make_async_copy(sinv.at[layer], sv, isem.at[1]))

    def u_copy(m):
        return pltpu.make_async_copy(ub, u_out.at[3 - m], usem.at[0])

    def precondition(m):
        ac, sc = inv_copies(m)
        ac.wait()
        sc.wait()

        @pl.when(m > 0)
        def _():
            u_copy(m - 1).wait()

        dw = pl.ds(pl.multiple_of(3 * m * UNIT, 8), D)

        def strip(i, carry):
            a = pl.ds(pl.multiple_of(i * BLK, 8), BLK)
            left = jnp.dot(av[a, :], pay[dw, :] * inv_tokens, precision=lax.Precision.HIGHEST,
                           preferred_element_type=jnp.float32)
            ub[a, :] = jnp.dot(left, sv[...], precision=lax.Precision.HIGHEST,
                               preferred_element_type=jnp.float32)
            return carry

        lax.fori_loop(0, 3, strip, 0)
        u_copy(m).start()

    def sym_copy(m):
        return pltpu.make_async_copy(rows_at(pay, base_of(m) * UNIT, 2 * UNIT), sym_out.at[m - 4], osem.at[m - 4])

    load(0, 0, 0)

    def tick(t, carry):
        for k in range(COPIES, 0, -1):
            m = t - k

            @pl.when(jnp.logical_and(m >= 0, m < MATS))
            def _(k=k, m=m):
                stage(k, m, 0)
                stage(k, m, 1)

                @pl.when(m < 4)
                def _():
                    stage(k, m, 2)
                    if k == COPIES - 1:
                        for c in inv_copies(m):
                            c.start()
                    if k == COPIES:
                        precondition(m)

                if k == COPIES:
                    @pl.when(m >= 4)
                    def _():
                        sym_copy(m).start()

        @pl.when(t < MATS)
        def _():
            @pl.when(t < 4)
            def _():
                gram_dw(t)

            @pl.when(t >= 4)
            def _():
                gram_sym(t)

            load(t + 1, 0, 0)
            scatter_copy(t, 0, 0).start()
            scatter_copy(t, 1, 0).start()

            @pl.when(t < 4)
            def _():
                scatter_copy(t, 2, 0).start()

        return carry

    lax.fori_loop(0, MATS + COPIES, tick, 0)
    u_copy(3).wait()

    def finish(m, carry):
        sym_copy(m).wait()
        return carry

    lax.fori_loop(4, MATS, finish, 0)


def reduce_all(arrays, ainv, sinv, tokens):
    any_spec = pl.BlockSpec(memory_space=pl.ANY)
    tok = arrays[0].shape[0]
    f32, bf16 = jnp.float32, jnp.bfloat16
    flops = 2 * tok * D * D * 10 + 8 * 12 * D ** 3
    return pl.pallas_call(
        functools.partial(reduce_kernel, 1.0 / tokens),
        out_shape=(jax.ShapeDtypeStruct((8, 2 * UNIT, D), f32), jax.ShapeDtypeStruct((LAYERS, D, D), f32)),
        in_specs=[any_spec] * 10,
        out_specs=(any_spec, any_spec),
        scratch_shapes=[
            pltpu.VMEM((UNITS * UNIT, D), f32),
            pltpu.VMEM((UNITS * RROWS, D), f32),
            pltpu.VMEM((2, tok // CHUNKS, D), bf16),
            pltpu.VMEM((2, tok // CHUNKS, D), bf16),
            pltpu.VMEM((D, D), f32),
            pltpu.VMEM((D, D), f32),
            pltpu.VMEM((D, D), f32),
            pltpu.SemaphoreType.DMA((MATS, 3, COPIES)),
            pltpu.SemaphoreType.DMA((MATS, 3, COPIES)),
            pltpu.SemaphoreType.REGULAR((MATS, 3, HALVINGS)),
            pltpu.SemaphoreType.DMA((2,)),
            pltpu.SemaphoreType.DMA((2,)),
            pltpu.SemaphoreType.DMA((2,)),
            pltpu.SemaphoreType.DMA((1,)),
            pltpu.SemaphoreType.DMA((8,)),
        ],
        compiler_params=pltpu.CompilerParams(collective_id=0, has_side_effects=True, vmem_limit_bytes=66 * 1000 * 1000),
        cost_estimate=pl.CostEstimate(flops=flops, bytes_accessed=8 * tok * D * 4, transcendentals=0),
        name="token_sums_reduced",
    )(*arrays, ainv, sinv)


def fold_kernel(scale, pa, ps, ao, so, an, sn):
    strip = pl.program_id(1)
    for packed, old, new in ((pa, ao, an), (ps, so, sn)):
        @pl.when(strip == 0)
        def _(packed=packed, old=old, new=new):
            new[0] = RHO * old[0] + scale * packed[0, 0:BLK, :]

        @pl.when(strip == 1)
        def _(packed=packed, old=old, new=new):
            new[0, :, 0:BLK] = RHO * old[0, :, 0:BLK] + scale * packed[0, 0:BLK, BLK:2 * BLK].T
            new[0, :, BLK:] = RHO * old[0, :, BLK:] + scale * packed[0, BLK:, 0:2 * BLK]

        @pl.when(strip == 2)
        def _(packed=packed, old=old, new=new):
            new[0, :, 0:BLK] = RHO * old[0, :, 0:BLK] + scale * packed[0, 0:BLK, 2 * BLK:].T
            new[0, :, BLK:2 * BLK] = RHO * old[0, :, BLK:2 * BLK] + scale * packed[0, BLK:, BLK:2 * BLK].T
            new[0, :, 2 * BLK:] = RHO * old[0, :, 2 * BLK:] + scale * packed[0, BLK:, 2 * BLK:]


def fold(packed, a_old, s_old, tokens):
    f32 = jnp.float32
    pack_a = pl.BlockSpec((1, 2 * UNIT, D), lambda l, i: (l, 0, 0))
    pack_s = pl.BlockSpec((1, 2 * UNIT, D), lambda l, i: (l + LAYERS, 0, 0))
    strip = pl.BlockSpec((1, BLK, D), lambda l, i: (l, i, 0))
    shape = jax.ShapeDtypeStruct((LAYERS, D, D), f32)
    return pl.pallas_call(
        functools.partial(fold_kernel, (1.0 - RHO) / tokens),
        out_shape=(shape, shape),
        grid=(LAYERS, 3),
        in_specs=[pack_a, pack_s, strip, strip],
        out_specs=(strip, strip),
        name="fold_factors",
    )(packed, packed, a_old, s_old)


def solution(mesh):
    group_size = mesh.shape["data"]

    def local_step(x_loc, dy_loc, w_stack, a_old, s_old, a_inv, s_inv):
        layers = w_stack.shape[0]
        tokens = x_loc.shape[0] * group_size
        acts = [x_loc]
        pre = []
        for i in range(layers - 1):
            z = jnp.dot(acts[-1], w_stack[i], preferred_element_type=jnp.float32).astype(jnp.bfloat16)
            pre.append(z)
            acts.append(gelu_fwd(z.astype(jnp.float32)).astype(jnp.bfloat16))
        grads = [None] * layers
        grads[-1] = dy_loc
        for i in reversed(range(layers - 1)):
            dh = times_wt(grads[i + 1], w_stack[i + 1]).astype(jnp.bfloat16)
            grads[i] = (dh.astype(jnp.float32) * gelu_slope(pre[i].astype(jnp.float32))).astype(jnp.bfloat16)
        packed, u_stack = reduce_all(acts + grads, a_inv, s_inv, tokens)
        a_new, s_new = fold(packed, a_old, s_old, tokens)
        return u_stack, a_new, s_new

    row_spec = P("data", None)
    full_spec = P()
    return jax.shard_map(local_step, mesh=mesh, in_specs=(row_spec, row_spec, full_spec, full_spec, full_spec, full_spec, full_spec), out_specs=(full_spec, full_spec, full_spec), check_vma=False)
```

```python
import functools

import jax
import jax.numpy as jnp
from jax import lax
from jax.experimental import pallas as pl
from jax.experimental.pallas import tpu as pltpu
from jax.sharding import PartitionSpec as P

RHO = 0.75
ERF_SCALE = 0.7071067811865476
PDF_SCALE = 0.3989422804014327

D = 768
BLK = 256
LAYERS = 4
UNIT = 256
HROWS = 384
MATS = 12
UNITS = 28
HALVINGS = 4
COPIES = 2 * HALVINGS + 1
RROWS = 256
MESH = pl.DeviceIdType.MESH
ORDERS = ((1, 2, 4, 8, 16), (1, 4, 2, 8, 16), (1, 8, 16, 2, 4))
CHUNKS = 4
LAG = (0, 1, 3, 5, 7, 9, 11, 13, 15, 16)
DN0 = (((0,), (0,)), ((), ()))


def gelu_fwd(z_val):
    return 0.5 * z_val * (1.0 + lax.erf(z_val * ERF_SCALE))


def gelu_slope(z_val):
    return 0.5 * (1.0 + lax.erf(z_val * ERF_SCALE)) + z_val * jnp.exp(-0.5 * z_val * z_val) * PDF_SCALE


def times_wt(g_rows, w_mat):
    return lax.dot_general(g_rows, w_mat, (((1,), (1,)), ((), ())), preferred_element_type=jnp.float32)


def half_of(step):
    return 128 >> step


def land_of(step):
    return 256 - (256 >> step)


def reduce_kernel(inv_tokens, x, h1, h2, h3, g1, g2, g3, dy, ainv, sinv,
                  sym_out, u_out,
                  pay, rbuf, lbuf, gbuf, av, sv, ub,
                  ssem, rsem, fsem, lsem, gsem, isem, usem, ussem, ursem, osem):
    me = lax.axis_index("data")
    tok = x.shape[0]
    chunk = tok // CHUNKS
    acts = (x, h1, h2, h3)
    grads = (g1, g2, g3, dy)

    def bit(mask):
        return lax.rem(lax.div(me, mask), 2)

    def peer(mask):
        return me + mask * (1 - 2 * bit(mask))

    barrier = pltpu.get_barrier_semaphore()
    for mask in ORDERS[0]:
        pl.semaphore_signal(barrier, inc=1, device_id=(peer(mask),), device_id_type=MESH)
    pl.semaphore_wait(barrier, 5)

    def offset(order, step):
        off = 0
        for s in range(step):
            off = off + bit(order[s]) * half_of(s)
        return off

    def base_of(m):
        late = lax.div(m + 8, 12)
        return 3 * m - late * (m - 4)

    def rows_at(ref, start, size):
        return ref.at[pl.ds(pl.multiple_of(start, 8), size), :]

    def scatter_copy(m, j, step):
        order = ORDERS[j]
        unit = base_of(m) + j
        half = half_of(step)
        b = bit(order[step])
        src = unit * UNIT + offset(order, step) + (1 - b) * half
        return pltpu.make_async_remote_copy(
            src_ref=rows_at(pay, src, half),
            dst_ref=rows_at(rbuf, unit * RROWS + land_of(step), half),
            send_sem=ssem.at[m, j, step], recv_sem=rsem.at[m, j, step],
            device_id=(peer(order[step]),), device_id_type=MESH)

    def exchange_copy(m, j):
        order = ORDERS[j]
        unit = base_of(m) + j
        return pltpu.make_async_remote_copy(
            src_ref=rows_at(pay, unit * UNIT + offset(order, HALVINGS), 16),
            dst_ref=rows_at(rbuf, unit * RROWS + 240, 16),
            send_sem=ssem.at[m, j, HALVINGS], recv_sem=rsem.at[m, j, HALVINGS],
            device_id=(peer(order[HALVINGS]),), device_id_type=MESH)

    def gather_copy(m, j, step):
        order = ORDERS[j]
        unit = base_of(m) + j
        half = half_of(step)
        row = unit * UNIT + offset(order, step + 1)
        return pltpu.make_async_remote_copy(
            src_ref=rows_at(pay, row, half),
            dst_ref=rows_at(pay, row, half),
            send_sem=ssem.at[m, j, HALVINGS + 1 + step], recv_sem=rsem.at[m, j, HALVINGS + 1 + step],
            device_id=(peer(order[step]),), device_id_type=MESH)

    def give_back(m, j, step):
        pl.semaphore_signal(fsem.at[m, j, step], inc=1, device_id=(peer(ORDERS[j][step]),), device_id_type=MESH)

    def gather_start(m, j, step):
        pl.semaphore_wait(fsem.at[m, j, step], 1)
        gather_copy(m, j, step).start()

    def add_landed(m, j, step):
        order = ORDERS[j]
        unit = base_of(m) + j
        half = half_of(step) if step < HALVINGS else 16
        keep = unit * UNIT + offset(order, min(step + 1, HALVINGS))
        land = unit * RROWS + land_of(step)
        piece = min(half, 32)

        def one(i, carry):
            a = pl.ds(pl.multiple_of(keep + i * piece, 8), piece)
            c = pl.ds(pl.multiple_of(land + i * piece, 8), piece)
            pay[a, :] = pay[a, :] + rbuf[c, :]
            return carry

        if half == piece:
            one(0, 0)
        else:
            lax.fori_loop(0, half // piece, one, 0)

    def stage(k, m, j):
        if k <= HALVINGS:
            scatter_copy(m, j, k - 1).wait()
            give_back(m, j, k - 1)
            add_landed(m, j, k - 1)
            if k < HALVINGS:
                scatter_copy(m, j, k).start()
            else:
                exchange_copy(m, j).start()
        elif k == HALVINGS + 1:
            exchange_copy(m, j).wait()
            add_landed(m, j, HALVINGS)
            gather_start(m, j, HALVINGS - 1)
        else:
            step = COPIES - k
            gather_copy(m, j, step).wait()
            if step > 0:
                gather_start(m, j, step - 1)

    def wait_left(kc, slot):
        pltpu.make_async_copy(x.at[pl.ds(kc * chunk, chunk), :], lbuf.at[slot], lsem.at[slot]).wait()

    def wait_right(kc, slot):
        pltpu.make_async_copy(dy.at[pl.ds(kc * chunk, chunk), :], gbuf.at[slot], gsem.at[slot]).wait()

    def load(m, kc, slot):
        rows = pl.ds(kc * chunk, chunk)
        for i in range(MATS):
            if i < 4:
                left, right = acts[3 - i], grads[3 - i]
            else:
                left, right = (acts + grads)[i - 4], None

            @pl.when(m == i)
            def _(left=left, right=right):
                pltpu.make_async_copy(left.at[rows, :], lbuf.at[slot], lsem.at[slot]).start()
                if right is not None:
                    pltpu.make_async_copy(right.at[rows, :], gbuf.at[slot], gsem.at[slot]).start()

    def put(first, row, rows, c0, cols, val):
        a = pl.ds(pl.multiple_of(row, 8), rows)
        if first:
            pay[a, c0:c0 + cols] = val
        else:
            pay[a, c0:c0 + cols] = pay[a, c0:c0 + cols] + val

    def gram_dw(m):
        row = base_of(m) * UNIT
        for kc in range(CHUNKS):
            slot = kc % 2
            wait_left(kc, slot)
            wait_right(kc, slot)
            if kc + 1 < CHUNKS:
                load(m, kc + 1, 1 - slot)
            for j in range(3):
                val = lax.dot_general(lbuf[slot, :, j * BLK:(j + 1) * BLK], gbuf[slot], DN0,
                                      preferred_element_type=jnp.float32)
                put(kc == 0, row + j * UNIT, UNIT, 0, D, val)

    def gram_sym(m):
        row = base_of(m) * UNIT
        for kc in range(CHUNKS):
            slot = kc % 2
            wait_left(kc, slot)
            if kc + 1 < CHUNKS:
                load(m, kc + 1, 1 - slot)
            for j, (unit, c0) in enumerate(((0, 0), (1, 0), (1, 2 * BLK))):
                cols = D - j * BLK
                val = lax.dot_general(lbuf[slot, :, j * BLK:(j + 1) * BLK], lbuf[slot, :, j * BLK:], DN0,
                                      preferred_element_type=jnp.float32)
                put(kc == 0, row + unit * UNIT, UNIT, c0, cols, val)

    own = pl.ds(pl.multiple_of(bit(1) * HROWS, 8), HROWS)

    def inv_copies(m):
        layer = 3 - m
        return (pltpu.make_async_copy(ainv.at[layer, own, :], av, isem.at[0]),
                pltpu.make_async_copy(sinv.at[layer], sv, isem.at[1]))

    def u_copies(m):
        dst = u_out.at[3 - m, own, :]
        return (pltpu.make_async_copy(ub, dst, usem.at[0]),
                pltpu.make_async_remote_copy(
                    src_ref=ub, dst_ref=dst, send_sem=ussem.at[m], recv_sem=ursem.at[m],
                    device_id=(peer(1),), device_id_type=MESH))

    def u_left(m):
        near, far = u_copies(m)
        near.wait()
        far.wait_send()

    def precondition(m):
        for c in inv_copies(m):
            c.wait()

        @pl.when(m > 0)
        def _():
            u_left(m - 1)

        dw = pl.ds(pl.multiple_of(3 * m * UNIT, 8), D)
        left = jnp.dot(av[...], pay[dw, :] * inv_tokens, precision=lax.Precision.HIGHEST,
                       preferred_element_type=jnp.float32)
        ub[...] = jnp.dot(left, sv[...], precision=lax.Precision.HIGHEST,
                          preferred_element_type=jnp.float32)
        for c in u_copies(m):
            c.start()

        @pl.when(m < 3)
        def _():
            for c in inv_copies(m + 1):
                c.start()

    def sym_copy(m):
        return pltpu.make_async_copy(rows_at(pay, base_of(m) * UNIT, 2 * UNIT), sym_out.at[m - 4], osem.at[m - 4])

    load(0, 0, 0)
    for c in inv_copies(0):
        c.start()

    def tick(t, carry):
        for k in range(COPIES, 0, -1):
            m = t - LAG[k]

            @pl.when(jnp.logical_and(m >= 0, m < MATS))
            def _(k=k, m=m):
                stage(k, m, 0)
                stage(k, m, 1)

                @pl.when(m < 4)
                def _():
                    stage(k, m, 2)
                    if k == COPIES:
                        precondition(m)

                if k == COPIES:
                    @pl.when(m >= 4)
                    def _():
                        sym_copy(m).start()

        @pl.when(t < MATS)
        def _():
            @pl.when(t < 4)
            def _():
                gram_dw(t)

            @pl.when(t >= 4)
            def _():
                gram_sym(t)

            load(t + 1, 0, 0)
            scatter_copy(t, 0, 0).start()
            scatter_copy(t, 1, 0).start()

            @pl.when(t < 4)
            def _():
                scatter_copy(t, 2, 0).start()

        return carry

    lax.fori_loop(0, MATS + LAG[COPIES], tick, 0)
    u_left(3)
    for m in range(LAYERS):
        u_copies(m)[1].wait_recv()

    def finish(m, carry):
        sym_copy(m).wait()
        return carry

    lax.fori_loop(4, MATS, finish, 0)


def reduce_all(arrays, ainv, sinv, tokens):
    any_spec = pl.BlockSpec(memory_space=pl.ANY)
    tok = arrays[0].shape[0]
    f32, bf16 = jnp.float32, jnp.bfloat16
    flops = 2 * tok * D * D * 10 + 8 * 12 * D ** 3
    return pl.pallas_call(
        functools.partial(reduce_kernel, 1.0 / tokens),
        out_shape=(jax.ShapeDtypeStruct((8, 2 * UNIT, D), f32), jax.ShapeDtypeStruct((LAYERS, D, D), f32)),
        in_specs=[any_spec] * 10,
        out_specs=(any_spec, any_spec),
        scratch_shapes=[
            pltpu.VMEM((UNITS * UNIT, D), f32),
            pltpu.VMEM((UNITS * RROWS, D), f32),
            pltpu.VMEM((2, tok // CHUNKS, D), bf16),
            pltpu.VMEM((2, tok // CHUNKS, D), bf16),
            pltpu.VMEM((HROWS, D), f32),
            pltpu.VMEM((D, D), f32),
            pltpu.VMEM((HROWS, D), f32),
            pltpu.SemaphoreType.DMA((MATS, 3, COPIES)),
            pltpu.SemaphoreType.DMA((MATS, 3, COPIES)),
            pltpu.SemaphoreType.REGULAR((MATS, 3, HALVINGS)),
            pltpu.SemaphoreType.DMA((2,)),
            pltpu.SemaphoreType.DMA((2,)),
            pltpu.SemaphoreType.DMA((2,)),
            pltpu.SemaphoreType.DMA((1,)),
            pltpu.SemaphoreType.DMA((LAYERS,)),
            pltpu.SemaphoreType.DMA((LAYERS,)),
            pltpu.SemaphoreType.DMA((8,)),
        ],
        compiler_params=pltpu.CompilerParams(collective_id=0, has_side_effects=True, vmem_limit_bytes=66 * 1000 * 1000),
        cost_estimate=pl.CostEstimate(flops=flops, bytes_accessed=8 * tok * D * 4, transcendentals=0),
        name="token_sums_reduced",
    )(*arrays, ainv, sinv)


def fold_kernel(scale, pa, ps, ao, so, an, sn):
    strip = pl.program_id(1)
    for packed, old, new in ((pa, ao, an), (ps, so, sn)):
        @pl.when(strip == 0)
        def _(packed=packed, old=old, new=new):
            new[0] = RHO * old[0] + scale * packed[0, 0:BLK, :]

        @pl.when(strip == 1)
        def _(packed=packed, old=old, new=new):
            new[0, :, 0:BLK] = RHO * old[0, :, 0:BLK] + scale * packed[0, 0:BLK, BLK:2 * BLK].T
            new[0, :, BLK:] = RHO * old[0, :, BLK:] + scale * packed[0, BLK:, 0:2 * BLK]

        @pl.when(strip == 2)
        def _(packed=packed, old=old, new=new):
            new[0, :, 0:BLK] = RHO * old[0, :, 0:BLK] + scale * packed[0, 0:BLK, 2 * BLK:].T
            new[0, :, BLK:2 * BLK] = RHO * old[0, :, BLK:2 * BLK] + scale * packed[0, BLK:, BLK:2 * BLK].T
            new[0, :, 2 * BLK:] = RHO * old[0, :, 2 * BLK:] + scale * packed[0, BLK:, 2 * BLK:]


def fold(packed, a_old, s_old, tokens):
    f32 = jnp.float32
    pack_a = pl.BlockSpec((1, 2 * UNIT, D), lambda l, i: (l, 0, 0))
    pack_s = pl.BlockSpec((1, 2 * UNIT, D), lambda l, i: (l + LAYERS, 0, 0))
    strip = pl.BlockSpec((1, BLK, D), lambda l, i: (l, i, 0))
    shape = jax.ShapeDtypeStruct((LAYERS, D, D), f32)
    return pl.pallas_call(
        functools.partial(fold_kernel, (1.0 - RHO) / tokens),
        out_shape=(shape, shape),
        grid=(LAYERS, 3),
        in_specs=[pack_a, pack_s, strip, strip],
        out_specs=(strip, strip),
        name="fold_factors",
    )(packed, packed, a_old, s_old)


def solution(mesh):
    group_size = mesh.shape["data"]

    def local_step(x_loc, dy_loc, w_stack, a_old, s_old, a_inv, s_inv):
        layers = w_stack.shape[0]
        tokens = x_loc.shape[0] * group_size
        acts = [x_loc]
        pre = []
        for i in range(layers - 1):
            z = jnp.dot(acts[-1], w_stack[i], preferred_element_type=jnp.float32).astype(jnp.bfloat16)
            pre.append(z)
            acts.append(gelu_fwd(z.astype(jnp.float32)).astype(jnp.bfloat16))
        grads = [None] * layers
        grads[-1] = dy_loc
        for i in reversed(range(layers - 1)):
            dh = times_wt(grads[i + 1], w_stack[i + 1]).astype(jnp.bfloat16)
            grads[i] = (dh.astype(jnp.float32) * gelu_slope(pre[i].astype(jnp.float32))).astype(jnp.bfloat16)
        packed, u_stack = reduce_all(acts + grads, a_inv, s_inv, tokens)
        a_new, s_new = fold(packed, a_old, s_old, tokens)
        return u_stack, a_new, s_new

    row_spec = P("data", None)
    full_spec = P()
    return jax.shard_map(local_step, mesh=mesh, in_specs=(row_spec, row_spec, full_spec, full_spec, full_spec, full_spec, full_spec), out_specs=(full_spec, full_spec, full_spec), check_vma=False)
```

```python
import functools

import jax
import jax.numpy as jnp
from jax import lax
from jax.experimental import pallas as pl
from jax.experimental.pallas import tpu as pltpu
from jax.sharding import PartitionSpec as P

RHO = 0.75
ERF_SCALE = 0.7071067811865476
PDF_SCALE = 0.3989422804014327

D = 768
BLK = 256
LAYERS = 4
UNIT = 256
HROWS = 384
MATS = 12
BLOCKS = 16
UNITS = 28
HALVINGS = 4
COPIES = 2 * HALVINGS + 1
RROWS = 256
MESH = pl.DeviceIdType.MESH
ORDERS = ((1, 2, 4, 8, 16), (1, 4, 2, 8, 16), (1, 8, 16, 2, 4))
CHUNKS = 4
ENTER = 18
PUMPS = ENTER + COPIES
DN0 = (((0,), (0,)), ((), ()))


def gelu_fwd(z_val):
    return 0.5 * z_val * (1.0 + lax.erf(z_val * ERF_SCALE))


def gelu_slope(z_val):
    return 0.5 * (1.0 + lax.erf(z_val * ERF_SCALE)) + z_val * jnp.exp(-0.5 * z_val * z_val) * PDF_SCALE


def times_wt(g_rows, w_mat):
    return lax.dot_general(g_rows, w_mat, (((1,), (1,)), ((), ())), preferred_element_type=jnp.float32)


def half_of(step):
    return 128 >> step


def land_of(step):
    return 256 - (256 >> step)


def reduce_kernel(inv_tokens, x, dy, w, ainv, sinv,
                  sym_out, u_out, hs, zs, gs,
                  pay, rbuf, lbuf, gbuf, av, sv, ub, wb, cin, cz, cout,
                  wsem, cisem, czsem, cosem,
                  ssem, rsem, fsem, lsem, gsem, isem, usem, ussem, ursem, osem):
    me = lax.axis_index("data")
    tok = x.shape[0]
    chunk = tok // CHUNKS
    acts = (x, hs.at[0], hs.at[1], hs.at[2])
    grads = (gs.at[0], gs.at[1], gs.at[2], dy)
    operands = ((dy, None), (x, None), (acts[1], None), (acts[2], None),
                (acts[3], dy), (acts[2], grads[2]), (acts[1], grads[1]), (x, grads[0]),
                (acts[3], None), (grads[2], None), (grads[1], None), (grads[0], None))

    def bit(mask):
        return lax.rem(lax.div(me, mask), 2)

    def peer(mask):
        return me + mask * (1 - 2 * bit(mask))

    barrier = pltpu.get_barrier_semaphore()
    for mask in ORDERS[0]:
        pl.semaphore_signal(barrier, inc=1, device_id=(peer(mask),), device_id_type=MESH)
    pl.semaphore_wait(barrier, 5)

    def offset(order, step):
        off = 0
        for s in range(step):
            off = off + bit(order[s]) * half_of(s)
        return off

    def base_of(m):
        return 2 * m + lax.div(m + 8, 12) * (m - 4) - lax.div(m + 4, 12) * (m - 8)

    def rows_at(ref, start, size):
        return ref.at[pl.ds(pl.multiple_of(start, 8), size), :]

    def scatter_copy(m, j, step):
        order = ORDERS[j]
        unit = base_of(m) + j
        half = half_of(step)
        b = bit(order[step])
        src = unit * UNIT + offset(order, step) + (1 - b) * half
        return pltpu.make_async_remote_copy(
            src_ref=rows_at(pay, src, half),
            dst_ref=rows_at(rbuf, unit * RROWS + land_of(step), half),
            send_sem=ssem.at[m, j, step], recv_sem=rsem.at[m, j, step],
            device_id=(peer(order[step]),), device_id_type=MESH)

    def exchange_copy(m, j):
        order = ORDERS[j]
        unit = base_of(m) + j
        return pltpu.make_async_remote_copy(
            src_ref=rows_at(pay, unit * UNIT + offset(order, HALVINGS), 16),
            dst_ref=rows_at(rbuf, unit * RROWS + 240, 16),
            send_sem=ssem.at[m, j, HALVINGS], recv_sem=rsem.at[m, j, HALVINGS],
            device_id=(peer(order[HALVINGS]),), device_id_type=MESH)

    def gather_copy(m, j, step):
        order = ORDERS[j]
        unit = base_of(m) + j
        half = half_of(step)
        row = unit * UNIT + offset(order, step + 1)
        return pltpu.make_async_remote_copy(
            src_ref=rows_at(pay, row, half),
            dst_ref=rows_at(pay, row, half),
            send_sem=ssem.at[m, j, HALVINGS + 1 + step], recv_sem=rsem.at[m, j, HALVINGS + 1 + step],
            device_id=(peer(order[step]),), device_id_type=MESH)

    def give_back(m, j, step):
        pl.semaphore_signal(fsem.at[m, j, step], inc=1, device_id=(peer(ORDERS[j][step]),), device_id_type=MESH)

    def gather_start(m, j, step):
        pl.semaphore_wait(fsem.at[m, j, step], 1)
        gather_copy(m, j, step).start()

    def add_landed(m, j, step):
        order = ORDERS[j]
        unit = base_of(m) + j
        half = half_of(step) if step < HALVINGS else 16
        keep = unit * UNIT + offset(order, min(step + 1, HALVINGS))
        land = unit * RROWS + land_of(step)
        piece = min(half, 32)

        def one(i, carry):
            a = pl.ds(pl.multiple_of(keep + i * piece, 8), piece)
            c = pl.ds(pl.multiple_of(land + i * piece, 8), piece)
            pay[a, :] = pay[a, :] + rbuf[c, :]
            return carry

        if half == piece:
            one(0, 0)
        else:
            lax.fori_loop(0, half // piece, one, 0)

    def stage(k, m, j):
        if k <= HALVINGS:
            scatter_copy(m, j, k - 1).wait()
            give_back(m, j, k - 1)
            add_landed(m, j, k - 1)
            if k < HALVINGS:
                scatter_copy(m, j, k).start()
            else:
                exchange_copy(m, j).start()
        elif k == HALVINGS + 1:
            exchange_copy(m, j).wait()
            add_landed(m, j, HALVINGS)
            gather_start(m, j, HALVINGS - 1)
        else:
            step = COPIES - k
            gather_copy(m, j, step).wait()
            if step > 0:
                gather_start(m, j, step - 1)

    def wait_left(kc, slot):
        pltpu.make_async_copy(x.at[pl.ds(kc * chunk, chunk), :], lbuf.at[slot], lsem.at[slot]).wait()

    def wait_right(kc, slot):
        pltpu.make_async_copy(dy.at[pl.ds(kc * chunk, chunk), :], gbuf.at[slot], gsem.at[slot]).wait()

    def load(m, kc, slot):
        rows = pl.ds(kc * chunk, chunk)
        for i in range(MATS):
            left, right = operands[i]

            @pl.when(m == i)
            def _(left=left, right=right):
                pltpu.make_async_copy(left.at[rows, :], lbuf.at[slot], lsem.at[slot]).start()
                if right is not None:
                    pltpu.make_async_copy(right.at[rows, :], gbuf.at[slot], gsem.at[slot]).start()

    def put(first, row, rows, c0, cols, val):
        a = pl.ds(pl.multiple_of(row, 8), rows)
        if first:
            pay[a, c0:c0 + cols] = val
        else:
            pay[a, c0:c0 + cols] = pay[a, c0:c0 + cols] + val

    def gram_dw(m):
        row = base_of(m) * UNIT
        for kc in range(CHUNKS):
            slot = kc % 2
            wait_left(kc, slot)
            wait_right(kc, slot)
            if kc + 1 < CHUNKS:
                load(m, kc + 1, 1 - slot)
            for j in range(3):
                val = lax.dot_general(lbuf[slot, :, j * BLK:(j + 1) * BLK], gbuf[slot], DN0,
                                      preferred_element_type=jnp.float32)
                put(kc == 0, row + j * UNIT, UNIT, 0, D, val)

    def gram_sym(m):
        row = base_of(m) * UNIT
        for kc in range(CHUNKS):
            slot = kc % 2
            wait_left(kc, slot)
            if kc + 1 < CHUNKS:
                load(m, kc + 1, 1 - slot)
            for j, (unit, c0) in enumerate(((0, 0), (1, 0), (1, 2 * BLK))):
                cols = D - j * BLK
                val = lax.dot_general(lbuf[slot, :, j * BLK:(j + 1) * BLK], lbuf[slot, :, j * BLK:], DN0,
                                      preferred_element_type=jnp.float32)
                put(kc == 0, row + unit * UNIT, UNIT, c0, cols, val)

    own = pl.ds(pl.multiple_of(bit(1) * HROWS, 8), HROWS)

    def inv_copies(m):
        layer = 3 - m
        return (pltpu.make_async_copy(ainv.at[layer, own, :], av, isem.at[0]),
                pltpu.make_async_copy(sinv.at[layer], sv, isem.at[1]))

    def u_copies(m):
        dst = u_out.at[3 - m, own, :]
        return (pltpu.make_async_copy(ub, dst, usem.at[0]),
                pltpu.make_async_remote_copy(
                    src_ref=ub, dst_ref=dst, send_sem=ussem.at[m], recv_sem=ursem.at[m],
                    device_id=(peer(1),), device_id_type=MESH))

    def u_left(m):
        near, far = u_copies(m)
        near.wait()
        far.wait_send()

    def precondition(m):
        for c in inv_copies(m):
            c.wait()

        @pl.when(m > 0)
        def _():
            u_left(m - 1)

        dw = pl.ds(pl.multiple_of((8 + 3 * m) * UNIT, 8), D)
        left = jnp.dot(av[...], pay[dw, :] * inv_tokens, precision=lax.Precision.HIGHEST,
                       preferred_element_type=jnp.float32)
        ub[...] = jnp.dot(left, sv[...], precision=lax.Precision.HIGHEST,
                          preferred_element_type=jnp.float32)
        for c in u_copies(m):
            c.start()

        @pl.when(m < 3)
        def _():
            for c in inv_copies(m + 1):
                c.start()

    def sym_copy(m):
        place = m - 4 * lax.div(m + 4, 12)
        return pltpu.make_async_copy(rows_at(pay, base_of(m) * UNIT, 2 * UNIT), sym_out.at[place], osem.at[place])

    block = tok // BLOCKS

    def block_rows(b):
        return pl.ds(pl.multiple_of(b * block, 8), block)

    def w_copy(step):
        layer = step + lax.div(step, 3) * (6 - 2 * step)
        return pltpu.make_async_copy(w.at[layer], wb.at[lax.rem(step, 2)], wsem.at[lax.rem(step, 2)])

    def w_next(step):
        w_copy(step).wait()

        @pl.when(step < 5)
        def _():
            w_copy(step + 1).start()

    def first_in(first, other, is_first, b, slot):
        @pl.when(is_first)
        def _():
            pltpu.make_async_copy(first.at[block_rows(b), :], cin.at[slot], cisem.at[slot]).start()

        @pl.when(jnp.logical_not(is_first))
        def _():
            pltpu.make_async_copy(other.at[block_rows(b), :], cin.at[slot], cisem.at[slot]).start()

    def z_in(i, b, slot):
        return pltpu.make_async_copy(zs.at[i, block_rows(b), :], cz.at[slot], czsem.at[slot])

    def z_out(i, b, slot):
        return pltpu.make_async_copy(cz.at[slot], zs.at[i, block_rows(b), :], czsem.at[slot])

    def out_copy(dst, b, slot):
        return pltpu.make_async_copy(cout.at[slot], dst.at[block_rows(b), :], cosem.at[slot])

    def forward(i):
        prev = hs.at[lax.rem(i + 2, 3)]
        dst = hs.at[i]
        w_next(i)
        weight = lax.rem(i, 2)
        first_in(x, prev, i == 0, 0, 0)

        def one(b, carry):
            slot = lax.rem(b, 2)

            @pl.when(b + 1 < BLOCKS)
            def _():
                first_in(x, prev, i == 0, b + 1, 1 - slot)

            pltpu.make_async_copy(x.at[block_rows(b), :], cin.at[slot], cisem.at[slot]).wait()

            @pl.when(b >= 2)
            def _():
                z_out(i, b - 2, slot).wait()
                out_copy(dst, b - 2, slot).wait()

            z_val = jnp.dot(cin[slot], wb[weight], preferred_element_type=jnp.float32).astype(jnp.bfloat16)
            cz[slot] = z_val
            cout[slot] = gelu_fwd(z_val.astype(jnp.float32)).astype(jnp.bfloat16)
            z_out(i, b, slot).start()
            out_copy(dst, b, slot).start()
            return carry

        lax.fori_loop(0, BLOCKS, one, 0)
        for b in (BLOCKS - 2, BLOCKS - 1):
            z_out(i, b, b % 2).wait()
            out_copy(dst, b, b % 2).wait()

    def backward(i):
        prev = gs.at[lax.rem(i + 1, 3)]
        dst = gs.at[i]
        step = 5 - i
        w_next(step)
        weight = lax.rem(step, 2)
        first_in(dy, prev, i == 2, 0, 0)
        z_in(i, 0, 0).start()

        def one(b, carry):
            slot = lax.rem(b, 2)

            @pl.when(b + 1 < BLOCKS)
            def _():
                first_in(dy, prev, i == 2, b + 1, 1 - slot)
                z_in(i, b + 1, 1 - slot).start()

            pltpu.make_async_copy(dy.at[block_rows(b), :], cin.at[slot], cisem.at[slot]).wait()
            z_in(i, b, slot).wait()

            @pl.when(b >= 2)
            def _():
                out_copy(dst, b - 2, slot).wait()

            dh = times_wt(cin[slot], wb[weight]).astype(jnp.bfloat16)
            cout[slot] = (dh.astype(jnp.float32) * gelu_slope(cz[slot].astype(jnp.float32))).astype(jnp.bfloat16)
            out_copy(dst, b, slot).start()
            return carry

        lax.fori_loop(0, BLOCKS, one, 0)
        for b in (BLOCKS - 2, BLOCKS - 1):
            out_copy(dst, b, b % 2).wait()

    def enters(e):
        return jnp.logical_and(jnp.logical_and(e >= 0, e < ENTER), jnp.logical_or(e >= 12, lax.rem(e, 2) == 0))

    def matrix(e):
        late = lax.div(e, 12)
        return (1 - late) * lax.div(e, 2) + late * (e - 6)

    def is_dw(m):
        return jnp.logical_and(m >= 4, m < 8)

    w_copy(0).start()
    load(0, 0, 0)
    for c in inv_copies(0):
        c.start()

    def pump(q, carry):
        for k in range(1, COPIES + 1):
            e = q - k

            @pl.when(enters(e))
            def _(k=k, e=e):
                m = matrix(e)
                stage(k, m, 0)
                stage(k, m, 1)

                @pl.when(is_dw(m))
                def _():
                    stage(k, m, 2)
                    if k == COPIES:
                        precondition(m - 4)

                if k == COPIES:
                    @pl.when(jnp.logical_not(is_dw(m)))
                    def _():
                        sym_copy(m).start()

        @pl.when(enters(q))
        def _():
            m = matrix(q)

            @pl.when(is_dw(m))
            def _():
                gram_dw(m)

            @pl.when(jnp.logical_not(is_dw(m)))
            def _():
                gram_sym(m)

            load(m + 1, 0, 0)
            scatter_copy(m, 0, 0).start()
            scatter_copy(m, 1, 0).start()

            @pl.when(is_dw(m))
            def _():
                scatter_copy(m, 2, 0).start()

        @pl.when(jnp.logical_and(q < 12, lax.rem(q, 2) == 1))
        def _():
            step = lax.div(q, 2)

            @pl.when(step < 3)
            def _():
                forward(step)

            @pl.when(step >= 3)
            def _():
                backward(5 - step)

        return carry

    lax.fori_loop(0, PUMPS, pump, 0)
    u_left(3)
    for m in range(LAYERS):
        u_copies(m)[1].wait_recv()

    for m in (0, 1, 2, 3, 8, 9, 10, 11):
        sym_copy(m).wait()


def reduce_all(x, dy, w, ainv, sinv, tokens):
    any_spec = pl.BlockSpec(memory_space=pl.ANY)
    tok = x.shape[0]
    f32, bf16 = jnp.float32, jnp.bfloat16
    flops = 2 * tok * D * D * 16 + 8 * 12 * D ** 3
    saved = jax.ShapeDtypeStruct((LAYERS - 1, tok, D), bf16)
    outs = pl.pallas_call(
        functools.partial(reduce_kernel, 1.0 / tokens),
        out_shape=(jax.ShapeDtypeStruct((8, 2 * UNIT, D), f32), jax.ShapeDtypeStruct((LAYERS, D, D), f32),
                   saved, saved, saved),
        in_specs=[any_spec] * 5,
        out_specs=(any_spec,) * 5,
        scratch_shapes=[
            pltpu.VMEM((UNITS * UNIT, D), f32),
            pltpu.VMEM((UNITS * RROWS, D), f32),
            pltpu.VMEM((2, tok // CHUNKS, D), bf16),
            pltpu.VMEM((2, tok // CHUNKS, D), bf16),
            pltpu.VMEM((HROWS, D), f32),
            pltpu.VMEM((D, D), f32),
            pltpu.VMEM((HROWS, D), f32),
            pltpu.VMEM((2, D, D), bf16),
            pltpu.VMEM((2, tok // BLOCKS, D), bf16),
            pltpu.VMEM((2, tok // BLOCKS, D), bf16),
            pltpu.VMEM((2, tok // BLOCKS, D), bf16),
            pltpu.SemaphoreType.DMA((2,)),
            pltpu.SemaphoreType.DMA((2,)),
            pltpu.SemaphoreType.DMA((2,)),
            pltpu.SemaphoreType.DMA((2,)),
            pltpu.SemaphoreType.DMA((MATS, 3, COPIES)),
            pltpu.SemaphoreType.DMA((MATS, 3, COPIES)),
            pltpu.SemaphoreType.REGULAR((MATS, 3, HALVINGS)),
            pltpu.SemaphoreType.DMA((2,)),
            pltpu.SemaphoreType.DMA((2,)),
            pltpu.SemaphoreType.DMA((2,)),
            pltpu.SemaphoreType.DMA((1,)),
            pltpu.SemaphoreType.DMA((LAYERS,)),
            pltpu.SemaphoreType.DMA((LAYERS,)),
            pltpu.SemaphoreType.DMA((8,)),
        ],
        compiler_params=pltpu.CompilerParams(collective_id=0, has_side_effects=True, vmem_limit_bytes=67 * 1000 * 1000),
        cost_estimate=pl.CostEstimate(flops=flops, bytes_accessed=16 * tok * D * 4, transcendentals=0),
        name="token_sums_reduced",
    )(x, dy, w, ainv, sinv)
    return outs[0], outs[1]


def fold_kernel(scale, pa, ps, ao, so, u_in, an, sn, u_out):
    strip = pl.program_id(1)
    u_out[...] = u_in[...]
    for packed, old, new in ((pa, ao, an), (ps, so, sn)):
        @pl.when(strip == 0)
        def _(packed=packed, old=old, new=new):
            new[0] = RHO * old[0] + scale * packed[0, 0:BLK, :]

        @pl.when(strip == 1)
        def _(packed=packed, old=old, new=new):
            new[0, :, 0:BLK] = RHO * old[0, :, 0:BLK] + scale * packed[0, 0:BLK, BLK:2 * BLK].T
            new[0, :, BLK:] = RHO * old[0, :, BLK:] + scale * packed[0, BLK:, 0:2 * BLK]

        @pl.when(strip == 2)
        def _(packed=packed, old=old, new=new):
            new[0, :, 0:BLK] = RHO * old[0, :, 0:BLK] + scale * packed[0, 0:BLK, 2 * BLK:].T
            new[0, :, BLK:2 * BLK] = RHO * old[0, :, BLK:2 * BLK] + scale * packed[0, BLK:, BLK:2 * BLK].T
            new[0, :, 2 * BLK:] = RHO * old[0, :, 2 * BLK:] + scale * packed[0, BLK:, 2 * BLK:]


def fold(packed, a_old, s_old, u_stack, tokens):
    f32 = jnp.float32
    pack_a = pl.BlockSpec((1, 2 * UNIT, D), lambda l, i: (l + 1, 0, 0))
    pack_s = pl.BlockSpec((1, 2 * UNIT, D), lambda l, i: ((7 - l) * (1 - l // 3), 0, 0))
    strip = pl.BlockSpec((1, BLK, D), lambda l, i: (l, i, 0))
    shape = jax.ShapeDtypeStruct((LAYERS, D, D), f32)
    return pl.pallas_call(
        functools.partial(fold_kernel, (1.0 - RHO) / tokens),
        out_shape=(shape, shape, shape),
        grid=(LAYERS, 3),
        in_specs=[pack_a, pack_s, strip, strip, strip],
        out_specs=(strip, strip, strip),
        name="fold_factors",
    )(packed, packed, a_old, s_old, u_stack)


def solution(mesh):
    group_size = mesh.shape["data"]

    def local_step(x_loc, dy_loc, w_stack, a_old, s_old, a_inv, s_inv):
        tokens = x_loc.shape[0] * group_size
        packed, u_stack = reduce_all(x_loc, dy_loc, w_stack, a_inv, s_inv, tokens)
        a_new, s_new, u_stack = fold(packed, a_old, s_old, u_stack, tokens)
        return u_stack, a_new, s_new

    row_spec = P("data", None)
    full_spec = P()
    return jax.shard_map(local_step, mesh=mesh, in_specs=(row_spec, row_spec, full_spec, full_spec, full_spec, full_spec, full_spec), out_specs=(full_spec, full_spec, full_spec), check_vma=False)
```

```python
import functools

import jax
import jax.numpy as jnp
from jax import lax
from jax.experimental import pallas as pl
from jax.experimental.pallas import tpu as pltpu
from jax.sharding import PartitionSpec as P

RHO = 0.75
ERF_SCALE = 0.7071067811865476
PDF_SCALE = 0.3989422804014327

D = 768
BLK = 256
LAYERS = 4
UNIT = 256
HROWS = 384
MATS = 12
BLOCKS = 16
UNITS = 28
HALVINGS = 4
COPIES = 2 * HALVINGS + 1
RROWS = 256
MESH = pl.DeviceIdType.MESH
ORDERS = ((1, 2, 4, 8, 16), (1, 4, 2, 8, 16), (1, 8, 16, 2, 4))
CHUNKS = 8
DEEP = 4
ENTER = 18
PUMPS = ENTER + COPIES
DN0 = (((0,), (0,)), ((), ()))


def gelu_fwd(z_val):
    return 0.5 * z_val * (1.0 + lax.erf(z_val * ERF_SCALE))


def gelu_slope(z_val):
    return 0.5 * (1.0 + lax.erf(z_val * ERF_SCALE)) + z_val * jnp.exp(-0.5 * z_val * z_val) * PDF_SCALE


def times_wt(g_rows, w_mat):
    return lax.dot_general(g_rows, w_mat, (((1,), (1,)), ((), ())), preferred_element_type=jnp.float32)


def half_of(step):
    return 128 >> step


def land_of(step):
    return 256 - (256 >> step)


def reduce_kernel(inv_tokens, x, dy, w, ainv, sinv,
                  sym_out, u_out, hs, zs, gs,
                  pay, rbuf, lbuf, gbuf, av, sv, ub, wb, cin, cz, cout,
                  wsem, cisem, czsem, cosem,
                  ssem, rsem, fsem, lsem, gsem, isem, usem, ussem, ursem, osem):
    me = lax.axis_index("data")
    tok = x.shape[0]
    chunk = tok // CHUNKS
    acts = (x, hs.at[0], hs.at[1], hs.at[2])
    grads = (gs.at[0], gs.at[1], gs.at[2], dy)
    operands = ((dy, None), (x, None), (acts[1], None), (acts[2], None),
                (acts[3], dy), (acts[2], grads[2]), (acts[1], grads[1]), (x, grads[0]),
                (acts[3], None), (grads[2], None), (grads[1], None), (grads[0], None))

    def bit(mask):
        return lax.rem(lax.div(me, mask), 2)

    def peer(mask):
        return me + mask * (1 - 2 * bit(mask))

    barrier = pltpu.get_barrier_semaphore()
    for mask in ORDERS[0]:
        pl.semaphore_signal(barrier, inc=1, device_id=(peer(mask),), device_id_type=MESH)
    pl.semaphore_wait(barrier, 5)

    def offset(order, step):
        off = 0
        for s in range(step):
            off = off + bit(order[s]) * half_of(s)
        return off

    def base_of(m):
        return 2 * m + lax.div(m + 8, 12) * (m - 4) - lax.div(m + 4, 12) * (m - 8)

    def rows_at(ref, start, size):
        return ref.at[pl.ds(pl.multiple_of(start, 8), size), :]

    def scatter_copy(m, j, step):
        order = ORDERS[j]
        unit = base_of(m) + j
        half = half_of(step)
        b = bit(order[step])
        src = unit * UNIT + offset(order, step) + (1 - b) * half
        return pltpu.make_async_remote_copy(
            src_ref=rows_at(pay, src, half),
            dst_ref=rows_at(rbuf, unit * RROWS + land_of(step), half),
            send_sem=ssem.at[m, j, step], recv_sem=rsem.at[m, j, step],
            device_id=(peer(order[step]),), device_id_type=MESH)

    def exchange_copy(m, j):
        order = ORDERS[j]
        unit = base_of(m) + j
        return pltpu.make_async_remote_copy(
            src_ref=rows_at(pay, unit * UNIT + offset(order, HALVINGS), 16),
            dst_ref=rows_at(rbuf, unit * RROWS + 240, 16),
            send_sem=ssem.at[m, j, HALVINGS], recv_sem=rsem.at[m, j, HALVINGS],
            device_id=(peer(order[HALVINGS]),), device_id_type=MESH)

    def gather_copy(m, j, step):
        order = ORDERS[j]
        unit = base_of(m) + j
        half = half_of(step)
        row = unit * UNIT + offset(order, step + 1)
        return pltpu.make_async_remote_copy(
            src_ref=rows_at(pay, row, half),
            dst_ref=rows_at(pay, row, half),
            send_sem=ssem.at[m, j, HALVINGS + 1 + step], recv_sem=rsem.at[m, j, HALVINGS + 1 + step],
            device_id=(peer(order[step]),), device_id_type=MESH)

    def give_back(m, j, step):
        pl.semaphore_signal(fsem.at[m, j, step], inc=1, device_id=(peer(ORDERS[j][step]),), device_id_type=MESH)

    def gather_start(m, j, step):
        pl.semaphore_wait(fsem.at[m, j, step], 1)
        gather_copy(m, j, step).start()

    def add_landed(m, j, step):
        order = ORDERS[j]
        unit = base_of(m) + j
        half = half_of(step) if step < HALVINGS else 16
        keep = unit * UNIT + offset(order, min(step + 1, HALVINGS))
        land = unit * RROWS + land_of(step)
        piece = min(half, 32)

        def one(i, carry):
            a = pl.ds(pl.multiple_of(keep + i * piece, 8), piece)
            c = pl.ds(pl.multiple_of(land + i * piece, 8), piece)
            pay[a, :] = pay[a, :] + rbuf[c, :]
            return carry

        if half == piece:
            one(0, 0)
        else:
            lax.fori_loop(0, half // piece, one, 0)

    def stage(k, m, j):
        if k <= HALVINGS:
            scatter_copy(m, j, k - 1).wait()
            give_back(m, j, k - 1)
            add_landed(m, j, k - 1)
            if k < HALVINGS:
                scatter_copy(m, j, k).start()
            else:
                exchange_copy(m, j).start()
        elif k == HALVINGS + 1:
            exchange_copy(m, j).wait()
            add_landed(m, j, HALVINGS)
            gather_start(m, j, HALVINGS - 1)
        else:
            step = COPIES - k
            gather_copy(m, j, step).wait()
            if step > 0:
                gather_start(m, j, step - 1)

    def wait_left(slot):
        pltpu.make_async_copy(x.at[pl.ds(0, chunk), :], lbuf.at[slot], lsem.at[slot]).wait()

    def wait_right(slot):
        pltpu.make_async_copy(dy.at[pl.ds(0, chunk), :], gbuf.at[slot], gsem.at[slot]).wait()

    def load(m, kc):
        rows = pl.ds(pl.multiple_of(kc * chunk, 8), chunk)
        slot = lax.rem(kc, DEEP)
        for i in range(MATS):
            left, right = operands[i]

            @pl.when(m == i)
            def _(left=left, right=right):
                pltpu.make_async_copy(left.at[rows, :], lbuf.at[slot], lsem.at[slot]).start()
                if right is not None:
                    pltpu.make_async_copy(right.at[rows, :], gbuf.at[slot], gsem.at[slot]).start()

    def put(first, row, rows, c0, cols, val):
        a = pl.ds(pl.multiple_of(row, 8), rows)
        if first:
            pay[a, c0:c0 + cols] = val
        else:
            pay[a, c0:c0 + cols] = pay[a, c0:c0 + cols] + val

    def gram(m, paired):
        row = base_of(m) * UNIT

        def piece(kc, first):
            slot = lax.rem(kc, DEEP)
            wait_left(slot)
            if paired:
                wait_right(slot)

            @pl.when(kc + DEEP - 1 < CHUNKS)
            def _():
                load(m, kc + DEEP - 1)

            if paired:
                for j in range(3):
                    val = lax.dot_general(lbuf[slot, :, j * BLK:(j + 1) * BLK], gbuf[slot], DN0,
                                          preferred_element_type=jnp.float32)
                    put(first, row + j * UNIT, UNIT, 0, D, val)
            else:
                for j, (unit, c0) in enumerate(((0, 0), (1, 0), (1, 2 * BLK))):
                    cols = D - j * BLK
                    val = lax.dot_general(lbuf[slot, :, j * BLK:(j + 1) * BLK], lbuf[slot, :, j * BLK:], DN0,
                                          preferred_element_type=jnp.float32)
                    put(first, row + unit * UNIT, UNIT, c0, cols, val)

        def rest(kc, carry):
            piece(kc, False)
            return carry

        piece(0, True)
        lax.fori_loop(1, CHUNKS, rest, 0)

    def load_first(m):
        for kc in range(DEEP - 1):
            load(m, kc)

    own = pl.ds(pl.multiple_of(bit(1) * HROWS, 8), HROWS)

    def inv_copies(m):
        layer = 3 - m
        return (pltpu.make_async_copy(ainv.at[layer, own, :], av, isem.at[0]),
                pltpu.make_async_copy(sinv.at[layer], sv, isem.at[1]))

    def u_copies(m):
        dst = u_out.at[3 - m, own, :]
        return (pltpu.make_async_copy(ub, dst, usem.at[0]),
                pltpu.make_async_remote_copy(
                    src_ref=ub, dst_ref=dst, send_sem=ussem.at[m], recv_sem=ursem.at[m],
                    device_id=(peer(1),), device_id_type=MESH))

    def u_left(m):
        near, far = u_copies(m)
        near.wait()
        far.wait_send()

    def precondition(m):
        for c in inv_copies(m):
            c.wait()

        @pl.when(m > 0)
        def _():
            u_left(m - 1)

        dw = pl.ds(pl.multiple_of((8 + 3 * m) * UNIT, 8), D)
        for r in (0, HROWS // 2):
            a = slice(r, r + HROWS // 2)
            left = inv_tokens * jnp.dot(av[a, :], pay[dw, :], precision=lax.Precision.HIGHEST,
                                        preferred_element_type=jnp.float32)
            ub[a, :] = jnp.dot(left, sv[...], precision=lax.Precision.HIGHEST,
                               preferred_element_type=jnp.float32)
        for c in u_copies(m):
            c.start()

        @pl.when(m < 3)
        def _():
            for c in inv_copies(m + 1):
                c.start()

    def sym_copy(m):
        place = m - 4 * lax.div(m + 4, 12)
        return pltpu.make_async_copy(rows_at(pay, base_of(m) * UNIT, 2 * UNIT), sym_out.at[place], osem.at[place])

    block = tok // BLOCKS

    def block_rows(b):
        return pl.ds(pl.multiple_of(b * block, 8), block)

    def w_copy(step):
        layer = step + lax.div(step, 3) * (6 - 2 * step)
        return pltpu.make_async_copy(w.at[layer], wb.at[lax.rem(step, 2)], wsem.at[lax.rem(step, 2)])

    def w_next(step):
        w_copy(step).wait()

        @pl.when(step < 5)
        def _():
            w_copy(step + 1).start()

    def first_in(first, other, is_first, b, slot):
        @pl.when(is_first)
        def _():
            pltpu.make_async_copy(first.at[block_rows(b), :], cin.at[slot], cisem.at[slot]).start()

        @pl.when(jnp.logical_not(is_first))
        def _():
            pltpu.make_async_copy(other.at[block_rows(b), :], cin.at[slot], cisem.at[slot]).start()

    def z_in(i, b, slot):
        return pltpu.make_async_copy(zs.at[i, block_rows(b), :], cz.at[slot], czsem.at[slot])

    def z_out(i, b, slot):
        return pltpu.make_async_copy(cz.at[slot], zs.at[i, block_rows(b), :], czsem.at[slot])

    def out_copy(dst, b, slot):
        return pltpu.make_async_copy(cout.at[slot], dst.at[block_rows(b), :], cosem.at[slot])

    def forward_first(i):
        prev = hs.at[lax.rem(i + 2, 3)]
        for b in range(DEEP - 1):
            first_in(x, prev, i == 0, b, b)

    def forward(i):
        prev = hs.at[lax.rem(i + 2, 3)]
        dst = hs.at[i]
        w_next(i)
        weight = lax.rem(i, 2)

        def one(b, carry):
            slot = lax.rem(b, DEEP)

            @pl.when(b + DEEP - 1 < BLOCKS)
            def _():
                first_in(x, prev, i == 0, b + DEEP - 1, lax.rem(b + DEEP - 1, DEEP))

            pltpu.make_async_copy(x.at[block_rows(b), :], cin.at[slot], cisem.at[slot]).wait()

            @pl.when(b >= DEEP)
            def _():
                z_out(i, b - DEEP, slot).wait()
                out_copy(dst, b - DEEP, slot).wait()

            z_val = jnp.dot(cin[slot], wb[weight], preferred_element_type=jnp.float32).astype(jnp.bfloat16)
            cz[slot] = z_val
            cout[slot] = gelu_fwd(z_val.astype(jnp.float32)).astype(jnp.bfloat16)
            z_out(i, b, slot).start()
            out_copy(dst, b, slot).start()
            return carry

        lax.fori_loop(0, BLOCKS, one, 0)
        for b in range(BLOCKS - DEEP, BLOCKS):
            z_out(i, b, b % DEEP).wait()
            out_copy(dst, b, b % DEEP).wait()

    def backward_first(i):
        prev = gs.at[lax.rem(i + 1, 3)]
        for b in range(DEEP - 1):
            first_in(dy, prev, i == 2, b, b)
            z_in(i, b, b).start()

    def backward(i):
        prev = gs.at[lax.rem(i + 1, 3)]
        dst = gs.at[i]
        step = 5 - i
        w_next(step)
        weight = lax.rem(step, 2)

        def one(b, carry):
            slot = lax.rem(b, DEEP)

            @pl.when(b + DEEP - 1 < BLOCKS)
            def _():
                ahead = lax.rem(b + DEEP - 1, DEEP)
                first_in(dy, prev, i == 2, b + DEEP - 1, ahead)
                z_in(i, b + DEEP - 1, ahead).start()

            pltpu.make_async_copy(dy.at[block_rows(b), :], cin.at[slot], cisem.at[slot]).wait()
            z_in(i, b, slot).wait()

            @pl.when(b >= DEEP)
            def _():
                out_copy(dst, b - DEEP, slot).wait()

            dh = times_wt(cin[slot], wb[weight]).astype(jnp.bfloat16)
            cout[slot] = (dh.astype(jnp.float32) * gelu_slope(cz[slot].astype(jnp.float32))).astype(jnp.bfloat16)
            out_copy(dst, b, slot).start()
            return carry

        lax.fori_loop(0, BLOCKS, one, 0)
        for b in range(BLOCKS - DEEP, BLOCKS):
            out_copy(dst, b, b % DEEP).wait()

    def enters(e):
        return jnp.logical_and(jnp.logical_and(e >= 0, e < ENTER), jnp.logical_or(e >= 12, lax.rem(e, 2) == 0))

    def matrix(e):
        late = lax.div(e, 12)
        return (1 - late) * lax.div(e, 2) + late * (e - 6)

    def is_dw(m):
        return jnp.logical_and(m >= 4, m < 8)

    w_copy(0).start()
    load_first(0)
    for c in inv_copies(0):
        c.start()

    def pump(q, carry):
        chained = jnp.logical_and(q < 12, lax.rem(q, 2) == 1)
        step = lax.div(q, 2)

        @pl.when(jnp.logical_and(chained, step < 3))
        def _():
            forward_first(step)

        @pl.when(jnp.logical_and(chained, step >= 3))
        def _():
            backward_first(5 - step)

        for k in range(1, COPIES + 1):
            e = q - k

            @pl.when(enters(e))
            def _(k=k, e=e):
                m = matrix(e)
                stage(k, m, 0)
                stage(k, m, 1)

                @pl.when(is_dw(m))
                def _():
                    stage(k, m, 2)
                    if k == COPIES:
                        precondition(m - 4)

                if k == COPIES:
                    @pl.when(jnp.logical_not(is_dw(m)))
                    def _():
                        sym_copy(m).start()

        @pl.when(enters(q))
        def _():
            m = matrix(q)

            @pl.when(is_dw(m))
            def _():
                gram(m, True)

            @pl.when(jnp.logical_not(is_dw(m)))
            def _():
                gram(m, False)

            load_first(m + 1)
            scatter_copy(m, 0, 0).start()
            scatter_copy(m, 1, 0).start()

            @pl.when(is_dw(m))
            def _():
                scatter_copy(m, 2, 0).start()

        @pl.when(jnp.logical_and(chained, step < 3))
        def _():
            forward(step)

        @pl.when(jnp.logical_and(chained, step >= 3))
        def _():
            backward(5 - step)

        return carry

    lax.fori_loop(0, PUMPS, pump, 0)
    u_left(3)
    for m in range(LAYERS):
        u_copies(m)[1].wait_recv()

    for m in (0, 1, 2, 3, 8, 9, 10, 11):
        sym_copy(m).wait()


def reduce_all(x, dy, w, ainv, sinv, tokens):
    any_spec = pl.BlockSpec(memory_space=pl.ANY)
    tok = x.shape[0]
    f32, bf16 = jnp.float32, jnp.bfloat16
    flops = 2 * tok * D * D * 16 + 8 * 12 * D ** 3
    saved = jax.ShapeDtypeStruct((LAYERS - 1, tok, D), bf16)
    outs = pl.pallas_call(
        functools.partial(reduce_kernel, 1.0 / tokens),
        out_shape=(jax.ShapeDtypeStruct((8, 2 * UNIT, D), f32), jax.ShapeDtypeStruct((LAYERS, D, D), f32),
                   saved, saved, saved),
        in_specs=[any_spec] * 5,
        out_specs=(any_spec,) * 5,
        scratch_shapes=[
            pltpu.VMEM((UNITS * UNIT, D), f32),
            pltpu.VMEM((UNITS * RROWS, D), f32),
            pltpu.VMEM((DEEP, tok // CHUNKS, D), bf16),
            pltpu.VMEM((DEEP, tok // CHUNKS, D), bf16),
            pltpu.VMEM((HROWS, D), f32),
            pltpu.VMEM((D, D), f32),
            pltpu.VMEM((HROWS, D), f32),
            pltpu.VMEM((2, D, D), bf16),
            pltpu.VMEM((DEEP, tok // BLOCKS, D), bf16),
            pltpu.VMEM((DEEP, tok // BLOCKS, D), bf16),
            pltpu.VMEM((DEEP, tok // BLOCKS, D), bf16),
            pltpu.SemaphoreType.DMA((2,)),
            pltpu.SemaphoreType.DMA((DEEP,)),
            pltpu.SemaphoreType.DMA((DEEP,)),
            pltpu.SemaphoreType.DMA((DEEP,)),
            pltpu.SemaphoreType.DMA((MATS, 3, COPIES)),
            pltpu.SemaphoreType.DMA((MATS, 3, COPIES)),
            pltpu.SemaphoreType.REGULAR((MATS, 3, HALVINGS)),
            pltpu.SemaphoreType.DMA((DEEP,)),
            pltpu.SemaphoreType.DMA((DEEP,)),
            pltpu.SemaphoreType.DMA((2,)),
            pltpu.SemaphoreType.DMA((1,)),
            pltpu.SemaphoreType.DMA((LAYERS,)),
            pltpu.SemaphoreType.DMA((LAYERS,)),
            pltpu.SemaphoreType.DMA((8,)),
        ],
        compiler_params=pltpu.CompilerParams(collective_id=0, has_side_effects=True, vmem_limit_bytes=67 * 1000 * 1000),
        cost_estimate=pl.CostEstimate(flops=flops, bytes_accessed=16 * tok * D * 4, transcendentals=0),
        name="token_sums_reduced",
    )(x, dy, w, ainv, sinv)
    return outs[0], outs[1]


def fold_kernel(scale, pa, ps, ao, so, u_in, an, sn, u_out):
    strip = pl.program_id(1)
    u_out[...] = u_in[...]
    for packed, old, new in ((pa, ao, an), (ps, so, sn)):
        @pl.when(strip == 0)
        def _(packed=packed, old=old, new=new):
            new[0] = RHO * old[0] + scale * packed[0, 0:BLK, :]

        @pl.when(strip == 1)
        def _(packed=packed, old=old, new=new):
            new[0, :, 0:BLK] = RHO * old[0, :, 0:BLK] + scale * packed[0, 0:BLK, BLK:2 * BLK].T
            new[0, :, BLK:] = RHO * old[0, :, BLK:] + scale * packed[0, BLK:, 0:2 * BLK]

        @pl.when(strip == 2)
        def _(packed=packed, old=old, new=new):
            new[0, :, 0:BLK] = RHO * old[0, :, 0:BLK] + scale * packed[0, 0:BLK, 2 * BLK:].T
            new[0, :, BLK:2 * BLK] = RHO * old[0, :, BLK:2 * BLK] + scale * packed[0, BLK:, BLK:2 * BLK].T
            new[0, :, 2 * BLK:] = RHO * old[0, :, 2 * BLK:] + scale * packed[0, BLK:, 2 * BLK:]


def fold(packed, a_old, s_old, u_stack, tokens):
    f32 = jnp.float32
    pack_a = pl.BlockSpec((1, 2 * UNIT, D), lambda l, i: (l + 1, 0, 0))
    pack_s = pl.BlockSpec((1, 2 * UNIT, D), lambda l, i: ((7 - l) * (1 - l // 3), 0, 0))
    strip = pl.BlockSpec((1, BLK, D), lambda l, i: (l, i, 0))
    shape = jax.ShapeDtypeStruct((LAYERS, D, D), f32)
    return pl.pallas_call(
        functools.partial(fold_kernel, (1.0 - RHO) / tokens),
        out_shape=(shape, shape, shape),
        grid=(LAYERS, 3),
        in_specs=[pack_a, pack_s, strip, strip, strip],
        out_specs=(strip, strip, strip),
        name="fold_factors",
    )(packed, packed, a_old, s_old, u_stack)


def solution(mesh):
    group_size = mesh.shape["data"]

    def local_step(x_loc, dy_loc, w_stack, a_old, s_old, a_inv, s_inv):
        tokens = x_loc.shape[0] * group_size
        packed, u_stack = reduce_all(x_loc, dy_loc, w_stack, a_inv, s_inv, tokens)
        a_new, s_new, u_stack = fold(packed, a_old, s_old, u_stack, tokens)
        return u_stack, a_new, s_new

    row_spec = P("data", None)
    full_spec = P()
    return jax.shard_map(local_step, mesh=mesh, in_specs=(row_spec, row_spec, full_spec, full_spec, full_spec, full_spec, full_spec), out_specs=(full_spec, full_spec, full_spec), check_vma=False)
```

```python
import functools

import jax
import jax.numpy as jnp
from jax import lax
from jax.experimental import pallas as pl
from jax.experimental.pallas import tpu as pltpu
from jax.sharding import PartitionSpec as P

RHO = 0.75
ERF_SCALE = 0.7071067811865476
PDF_SCALE = 0.3989422804014327

D = 768
BLK = 256
LAYERS = 4
UNIT = 256
HROWS = 384
MATS = 12
BLOCKS = 16
UNITS = 28
HALVINGS = 4
COPIES = 2 * HALVINGS + 1
RROWS = 256
MESH = pl.DeviceIdType.MESH
ORDERS = ((1, 2, 4, 8, 16), (1, 4, 2, 8, 16), (1, 8, 16, 2, 4))
CHUNKS = 8
DEEP = 4
ENTER = 18
LAG = (0, 2, 4, 5, 6, 7, 8, 9, 11, 12)
PUMPS = ENTER + LAG[COPIES]
DN0 = (((0,), (0,)), ((), ()))


def gelu_fwd(z_val):
    return 0.5 * z_val * (1.0 + lax.erf(z_val * ERF_SCALE))


def gelu_slope(z_val):
    return 0.5 * (1.0 + lax.erf(z_val * ERF_SCALE)) + z_val * jnp.exp(-0.5 * z_val * z_val) * PDF_SCALE


def times_wt(g_rows, w_mat):
    return lax.dot_general(g_rows, w_mat, (((1,), (1,)), ((), ())), preferred_element_type=jnp.float32)


def half_of(step):
    return 128 >> step


def land_of(step):
    return 256 - (256 >> step)


def reduce_kernel(inv_tokens, x, dy, w, ainv, sinv,
                  sym_out, u_out, hs, zs, gs,
                  pay, rbuf, lbuf, gbuf, av, sv, ub, wb, cin, cz, cout,
                  wsem, cisem, czsem, cosem,
                  ssem, rsem, fsem, lsem, gsem, isem, usem, ussem, ursem, osem):
    me = lax.axis_index("data")
    tok = x.shape[0]
    chunk = tok // CHUNKS
    acts = (x, hs.at[0], hs.at[1], hs.at[2])
    grads = (gs.at[0], gs.at[1], gs.at[2], dy)
    operands = ((dy, None), (x, None), (acts[1], None), (acts[2], None),
                (acts[3], dy), (acts[2], grads[2]), (acts[1], grads[1]), (x, grads[0]),
                (acts[3], None), (grads[2], None), (grads[1], None), (grads[0], None))

    def bit(mask):
        return lax.rem(lax.div(me, mask), 2)

    def peer(mask):
        return me + mask * (1 - 2 * bit(mask))

    barrier = pltpu.get_barrier_semaphore()
    for mask in ORDERS[0]:
        pl.semaphore_signal(barrier, inc=1, device_id=(peer(mask),), device_id_type=MESH)
    pl.semaphore_wait(barrier, 5)

    def offset(order, step):
        off = 0
        for s in range(step):
            off = off + bit(order[s]) * half_of(s)
        return off

    def base_of(m):
        return 2 * m + lax.div(m + 8, 12) * (m - 4) - lax.div(m + 4, 12) * (m - 8)

    def rows_at(ref, start, size):
        return ref.at[pl.ds(pl.multiple_of(start, 8), size), :]

    def scatter_copy(m, j, step):
        order = ORDERS[j]
        unit = base_of(m) + j
        half = half_of(step)
        b = bit(order[step])
        src = unit * UNIT + offset(order, step) + (1 - b) * half
        return pltpu.make_async_remote_copy(
            src_ref=rows_at(pay, src, half),
            dst_ref=rows_at(rbuf, unit * RROWS + land_of(step), half),
            send_sem=ssem.at[m, j, step], recv_sem=rsem.at[m, j, step],
            device_id=(peer(order[step]),), device_id_type=MESH)

    def exchange_copy(m, j):
        order = ORDERS[j]
        unit = base_of(m) + j
        return pltpu.make_async_remote_copy(
            src_ref=rows_at(pay, unit * UNIT + offset(order, HALVINGS), 16),
            dst_ref=rows_at(rbuf, unit * RROWS + 240, 16),
            send_sem=ssem.at[m, j, HALVINGS], recv_sem=rsem.at[m, j, HALVINGS],
            device_id=(peer(order[HALVINGS]),), device_id_type=MESH)

    def gather_copy(m, j, step):
        order = ORDERS[j]
        unit = base_of(m) + j
        half = half_of(step)
        row = unit * UNIT + offset(order, step + 1)
        return pltpu.make_async_remote_copy(
            src_ref=rows_at(pay, row, half),
            dst_ref=rows_at(pay, row, half),
            send_sem=ssem.at[m, j, HALVINGS + 1 + step], recv_sem=rsem.at[m, j, HALVINGS + 1 + step],
            device_id=(peer(order[step]),), device_id_type=MESH)

    def give_back(m, j, step):
        pl.semaphore_signal(fsem.at[m, j, step], inc=1, device_id=(peer(ORDERS[j][step]),), device_id_type=MESH)

    def gather_start(m, j, step):
        pl.semaphore_wait(fsem.at[m, j, step], 1)
        gather_copy(m, j, step).start()

    def add_landed(m, j, step):
        order = ORDERS[j]
        unit = base_of(m) + j
        half = half_of(step) if step < HALVINGS else 16
        keep = unit * UNIT + offset(order, min(step + 1, HALVINGS))
        land = unit * RROWS + land_of(step)
        piece = min(half, 32)

        def one(i, carry):
            a = pl.ds(pl.multiple_of(keep + i * piece, 8), piece)
            c = pl.ds(pl.multiple_of(land + i * piece, 8), piece)
            pay[a, :] = pay[a, :] + rbuf[c, :]
            return carry

        if half == piece:
            one(0, 0)
        else:
            lax.fori_loop(0, half // piece, one, 0)

    def stage(k, m, j):
        if k <= HALVINGS:
            scatter_copy(m, j, k - 1).wait()
            give_back(m, j, k - 1)
            add_landed(m, j, k - 1)
            if k < HALVINGS:
                scatter_copy(m, j, k).start()
            else:
                exchange_copy(m, j).start()
        elif k == HALVINGS + 1:
            exchange_copy(m, j).wait()
            add_landed(m, j, HALVINGS)
            gather_start(m, j, HALVINGS - 1)
        else:
            step = COPIES - k
            gather_copy(m, j, step).wait()
            if step > 0:
                gather_start(m, j, step - 1)

    def wait_left(slot):
        pltpu.make_async_copy(x.at[pl.ds(0, chunk), :], lbuf.at[slot], lsem.at[slot]).wait()

    def wait_right(slot):
        pltpu.make_async_copy(dy.at[pl.ds(0, chunk), :], gbuf.at[slot], gsem.at[slot]).wait()

    def load(m, kc):
        rows = pl.ds(pl.multiple_of(kc * chunk, 8), chunk)
        slot = lax.rem(kc, DEEP)
        for i in range(MATS):
            left, right = operands[i]

            @pl.when(m == i)
            def _(left=left, right=right):
                pltpu.make_async_copy(left.at[rows, :], lbuf.at[slot], lsem.at[slot]).start()
                if right is not None:
                    pltpu.make_async_copy(right.at[rows, :], gbuf.at[slot], gsem.at[slot]).start()

    def put(first, row, rows, c0, cols, val):
        a = pl.ds(pl.multiple_of(row, 8), rows)
        if first:
            pay[a, c0:c0 + cols] = val
        else:
            pay[a, c0:c0 + cols] = pay[a, c0:c0 + cols] + val

    def gram(m, paired):
        row = base_of(m) * UNIT

        def piece(kc, first):
            slot = lax.rem(kc, DEEP)
            wait_left(slot)
            if paired:
                wait_right(slot)

            @pl.when(kc + DEEP - 1 < CHUNKS)
            def _():
                load(m, kc + DEEP - 1)

            if paired:
                for j in range(3):
                    val = lax.dot_general(lbuf[slot, :, j * BLK:(j + 1) * BLK], gbuf[slot], DN0,
                                          preferred_element_type=jnp.float32)
                    put(first, row + j * UNIT, UNIT, 0, D, val)
            else:
                for j, (unit, c0) in enumerate(((0, 0), (1, 0), (1, 2 * BLK))):
                    cols = D - j * BLK
                    val = lax.dot_general(lbuf[slot, :, j * BLK:(j + 1) * BLK], lbuf[slot, :, j * BLK:], DN0,
                                          preferred_element_type=jnp.float32)
                    put(first, row + unit * UNIT, UNIT, c0, cols, val)

        def rest(kc, carry):
            piece(kc, False)
            return carry

        piece(0, True)
        lax.fori_loop(1, CHUNKS, rest, 0)

    def load_first(m):
        for kc in range(DEEP - 1):
            load(m, kc)

    own = pl.ds(pl.multiple_of(bit(1) * HROWS, 8), HROWS)

    def inv_copies(m):
        layer = 3 - m
        return (pltpu.make_async_copy(ainv.at[layer, own, :], av, isem.at[0]),
                pltpu.make_async_copy(sinv.at[layer], sv, isem.at[1]))

    def u_copies(m):
        dst = u_out.at[3 - m, own, :]
        return (pltpu.make_async_copy(ub, dst, usem.at[0]),
                pltpu.make_async_remote_copy(
                    src_ref=ub, dst_ref=dst, send_sem=ussem.at[m], recv_sem=ursem.at[m],
                    device_id=(peer(1),), device_id_type=MESH))

    def u_left(m):
        near, far = u_copies(m)
        near.wait()
        far.wait_send()

    def precondition(m):
        for c in inv_copies(m):
            c.wait()

        @pl.when(m > 0)
        def _():
            u_left(m - 1)

        dw = pl.ds(pl.multiple_of((8 + 3 * m) * UNIT, 8), D)
        for r in (0, HROWS // 2):
            a = slice(r, r + HROWS // 2)
            left = inv_tokens * jnp.dot(av[a, :], pay[dw, :], precision=lax.Precision.HIGHEST,
                                        preferred_element_type=jnp.float32)
            ub[a, :] = jnp.dot(left, sv[...], precision=lax.Precision.HIGHEST,
                               preferred_element_type=jnp.float32)
        for c in u_copies(m):
            c.start()

        @pl.when(m < 3)
        def _():
            for c in inv_copies(m + 1):
                c.start()

    def sym_copy(m):
        place = m - 4 * lax.div(m + 4, 12)
        return pltpu.make_async_copy(rows_at(pay, base_of(m) * UNIT, 2 * UNIT), sym_out.at[place], osem.at[place])

    block = tok // BLOCKS

    def block_rows(b):
        return pl.ds(pl.multiple_of(b * block, 8), block)

    def w_copy(step):
        layer = step + lax.div(step, 3) * (6 - 2 * step)
        return pltpu.make_async_copy(w.at[layer], wb.at[lax.rem(step, 2)], wsem.at[lax.rem(step, 2)])

    def w_next(step):
        w_copy(step).wait()

        @pl.when(step < 5)
        def _():
            w_copy(step + 1).start()

    def first_in(first, other, is_first, b, slot):
        @pl.when(is_first)
        def _():
            pltpu.make_async_copy(first.at[block_rows(b), :], cin.at[slot], cisem.at[slot]).start()

        @pl.when(jnp.logical_not(is_first))
        def _():
            pltpu.make_async_copy(other.at[block_rows(b), :], cin.at[slot], cisem.at[slot]).start()

    def z_in(i, b, slot):
        return pltpu.make_async_copy(zs.at[i, block_rows(b), :], cz.at[slot], czsem.at[slot])

    def z_out(i, b, slot):
        return pltpu.make_async_copy(cz.at[slot], zs.at[i, block_rows(b), :], czsem.at[slot])

    def out_copy(dst, b, slot):
        return pltpu.make_async_copy(cout.at[slot], dst.at[block_rows(b), :], cosem.at[slot])

    def forward_first(i):
        prev = hs.at[lax.rem(i + 2, 3)]
        for b in range(DEEP - 1):
            first_in(x, prev, i == 0, b, b)

    def forward(i):
        prev = hs.at[lax.rem(i + 2, 3)]
        dst = hs.at[i]
        w_next(i)
        weight = lax.rem(i, 2)

        def one(b, carry):
            slot = lax.rem(b, DEEP)

            @pl.when(b + DEEP - 1 < BLOCKS)
            def _():
                first_in(x, prev, i == 0, b + DEEP - 1, lax.rem(b + DEEP - 1, DEEP))

            pltpu.make_async_copy(x.at[block_rows(b), :], cin.at[slot], cisem.at[slot]).wait()

            @pl.when(b >= DEEP)
            def _():
                z_out(i, b - DEEP, slot).wait()
                out_copy(dst, b - DEEP, slot).wait()

            z_val = jnp.dot(cin[slot], wb[weight], preferred_element_type=jnp.float32).astype(jnp.bfloat16)
            cz[slot] = z_val
            cout[slot] = gelu_fwd(z_val.astype(jnp.float32)).astype(jnp.bfloat16)
            z_out(i, b, slot).start()
            out_copy(dst, b, slot).start()
            return carry

        lax.fori_loop(0, BLOCKS, one, 0)
        for b in range(BLOCKS - DEEP, BLOCKS):
            z_out(i, b, b % DEEP).wait()
            out_copy(dst, b, b % DEEP).wait()

    def backward_first(i):
        prev = gs.at[lax.rem(i + 1, 3)]
        for b in range(DEEP - 1):
            first_in(dy, prev, i == 2, b, b)
            z_in(i, b, b).start()

    def backward(i):
        prev = gs.at[lax.rem(i + 1, 3)]
        dst = gs.at[i]
        step = 5 - i
        w_next(step)
        weight = lax.rem(step, 2)

        def one(b, carry):
            slot = lax.rem(b, DEEP)

            @pl.when(b + DEEP - 1 < BLOCKS)
            def _():
                ahead = lax.rem(b + DEEP - 1, DEEP)
                first_in(dy, prev, i == 2, b + DEEP - 1, ahead)
                z_in(i, b + DEEP - 1, ahead).start()

            pltpu.make_async_copy(dy.at[block_rows(b), :], cin.at[slot], cisem.at[slot]).wait()
            z_in(i, b, slot).wait()

            @pl.when(b >= DEEP)
            def _():
                out_copy(dst, b - DEEP, slot).wait()

            dh = times_wt(cin[slot], wb[weight]).astype(jnp.bfloat16)
            cout[slot] = (dh.astype(jnp.float32) * gelu_slope(cz[slot].astype(jnp.float32))).astype(jnp.bfloat16)
            out_copy(dst, b, slot).start()
            return carry

        lax.fori_loop(0, BLOCKS, one, 0)
        for b in range(BLOCKS - DEEP, BLOCKS):
            out_copy(dst, b, b % DEEP).wait()

    def enters(e):
        return jnp.logical_and(jnp.logical_and(e >= 0, e < ENTER), jnp.logical_or(e >= 12, lax.rem(e, 2) == 0))

    def matrix(e):
        late = lax.div(e, 12)
        return (1 - late) * lax.div(e, 2) + late * (e - 6)

    def is_dw(m):
        return jnp.logical_and(m >= 4, m < 8)

    w_copy(0).start()
    load_first(0)
    for c in inv_copies(0):
        c.start()

    def pump(q, carry):
        chained = jnp.logical_and(q < 12, lax.rem(q, 2) == 1)
        step = lax.div(q, 2)

        @pl.when(jnp.logical_and(chained, step < 3))
        def _():
            forward_first(step)

        @pl.when(jnp.logical_and(chained, step >= 3))
        def _():
            backward_first(5 - step)

        for k in range(1, COPIES + 1):
            e = q - LAG[k]

            @pl.when(enters(e))
            def _(k=k, e=e):
                m = matrix(e)
                stage(k, m, 0)
                stage(k, m, 1)

                @pl.when(is_dw(m))
                def _():
                    stage(k, m, 2)
                    if k == COPIES:
                        precondition(m - 4)

                if k == COPIES:
                    @pl.when(jnp.logical_not(is_dw(m)))
                    def _():
                        sym_copy(m).start()

        @pl.when(enters(q))
        def _():
            m = matrix(q)

            @pl.when(is_dw(m))
            def _():
                gram(m, True)

            @pl.when(jnp.logical_not(is_dw(m)))
            def _():
                gram(m, False)

            load_first(m + 1)
            scatter_copy(m, 0, 0).start()
            scatter_copy(m, 1, 0).start()

            @pl.when(is_dw(m))
            def _():
                scatter_copy(m, 2, 0).start()

        @pl.when(jnp.logical_and(chained, step < 3))
        def _():
            forward(step)

        @pl.when(jnp.logical_and(chained, step >= 3))
        def _():
            backward(5 - step)

        return carry

    lax.fori_loop(0, PUMPS, pump, 0)
    u_left(3)
    for m in range(LAYERS):
        u_copies(m)[1].wait_recv()

    for m in (0, 1, 2, 3, 8, 9, 10, 11):
        sym_copy(m).wait()


def reduce_all(x, dy, w, ainv, sinv, tokens):
    any_spec = pl.BlockSpec(memory_space=pl.ANY)
    tok = x.shape[0]
    f32, bf16 = jnp.float32, jnp.bfloat16
    flops = 2 * tok * D * D * 16 + 8 * 12 * D ** 3
    saved = jax.ShapeDtypeStruct((LAYERS - 1, tok, D), bf16)
    outs = pl.pallas_call(
        functools.partial(reduce_kernel, 1.0 / tokens),
        out_shape=(jax.ShapeDtypeStruct((8, 2 * UNIT, D), f32), jax.ShapeDtypeStruct((LAYERS, D, D), f32),
                   saved, saved, saved),
        in_specs=[any_spec] * 5,
        out_specs=(any_spec,) * 5,
        scratch_shapes=[
            pltpu.VMEM((UNITS * UNIT, D), f32),
            pltpu.VMEM((UNITS * RROWS, D), f32),
            pltpu.VMEM((DEEP, tok // CHUNKS, D), bf16),
            pltpu.VMEM((DEEP, tok // CHUNKS, D), bf16),
            pltpu.VMEM((HROWS, D), f32),
            pltpu.VMEM((D, D), f32),
            pltpu.VMEM((HROWS, D), f32),
            pltpu.VMEM((2, D, D), bf16),
            pltpu.VMEM((DEEP, tok // BLOCKS, D), bf16),
            pltpu.VMEM((DEEP, tok // BLOCKS, D), bf16),
            pltpu.VMEM((DEEP, tok // BLOCKS, D), bf16),
            pltpu.SemaphoreType.DMA((2,)),
            pltpu.SemaphoreType.DMA((DEEP,)),
            pltpu.SemaphoreType.DMA((DEEP,)),
            pltpu.SemaphoreType.DMA((DEEP,)),
            pltpu.SemaphoreType.DMA((MATS, 3, COPIES)),
            pltpu.SemaphoreType.DMA((MATS, 3, COPIES)),
            pltpu.SemaphoreType.REGULAR((MATS, 3, HALVINGS)),
            pltpu.SemaphoreType.DMA((DEEP,)),
            pltpu.SemaphoreType.DMA((DEEP,)),
            pltpu.SemaphoreType.DMA((2,)),
            pltpu.SemaphoreType.DMA((1,)),
            pltpu.SemaphoreType.DMA((LAYERS,)),
            pltpu.SemaphoreType.DMA((LAYERS,)),
            pltpu.SemaphoreType.DMA((8,)),
        ],
        compiler_params=pltpu.CompilerParams(collective_id=0, has_side_effects=True, vmem_limit_bytes=67 * 1000 * 1000),
        cost_estimate=pl.CostEstimate(flops=flops, bytes_accessed=16 * tok * D * 4, transcendentals=0),
        name="token_sums_reduced",
    )(x, dy, w, ainv, sinv)
    return outs[0], outs[1]


def fold_kernel(scale, pa, ps, ao, so, u_in, an, sn, u_out):
    strip = pl.program_id(1)
    u_out[...] = u_in[...]
    for packed, old, new in ((pa, ao, an), (ps, so, sn)):
        @pl.when(strip == 0)
        def _(packed=packed, old=old, new=new):
            new[0] = RHO * old[0] + scale * packed[0, 0:BLK, :]

        @pl.when(strip == 1)
        def _(packed=packed, old=old, new=new):
            new[0, :, 0:BLK] = RHO * old[0, :, 0:BLK] + scale * packed[0, 0:BLK, BLK:2 * BLK].T
            new[0, :, BLK:] = RHO * old[0, :, BLK:] + scale * packed[0, BLK:, 0:2 * BLK]

        @pl.when(strip == 2)
        def _(packed=packed, old=old, new=new):
            new[0, :, 0:BLK] = RHO * old[0, :, 0:BLK] + scale * packed[0, 0:BLK, 2 * BLK:].T
            new[0, :, BLK:2 * BLK] = RHO * old[0, :, BLK:2 * BLK] + scale * packed[0, BLK:, BLK:2 * BLK].T
            new[0, :, 2 * BLK:] = RHO * old[0, :, 2 * BLK:] + scale * packed[0, BLK:, 2 * BLK:]


def fold(packed, a_old, s_old, u_stack, tokens):
    f32 = jnp.float32
    pack_a = pl.BlockSpec((1, 2 * UNIT, D), lambda l, i: (l + 1, 0, 0))
    pack_s = pl.BlockSpec((1, 2 * UNIT, D), lambda l, i: ((7 - l) * (1 - l // 3), 0, 0))
    strip = pl.BlockSpec((1, BLK, D), lambda l, i: (l, i, 0))
    shape = jax.ShapeDtypeStruct((LAYERS, D, D), f32)
    return pl.pallas_call(
        functools.partial(fold_kernel, (1.0 - RHO) / tokens),
        out_shape=(shape, shape, shape),
        grid=(LAYERS, 3),
        in_specs=[pack_a, pack_s, strip, strip, strip],
        out_specs=(strip, strip, strip),
        name="fold_factors",
    )(packed, packed, a_old, s_old, u_stack)


def solution(mesh):
    group_size = mesh.shape["data"]

    def local_step(x_loc, dy_loc, w_stack, a_old, s_old, a_inv, s_inv):
        tokens = x_loc.shape[0] * group_size
        packed, u_stack = reduce_all(x_loc, dy_loc, w_stack, a_inv, s_inv, tokens)
        a_new, s_new, u_stack = fold(packed, a_old, s_old, u_stack, tokens)
        return u_stack, a_new, s_new

    row_spec = P("data", None)
    full_spec = P()
    return jax.shard_map(local_step, mesh=mesh, in_specs=(row_spec, row_spec, full_spec, full_spec, full_spec, full_spec, full_spec), out_specs=(full_spec, full_spec, full_spec), check_vma=False)
```
